8 devices in a mesh: tp: 2 (over z, y), dp: 4 (over x, core).
Axes of the slice: x: 2, y: 2, z: 1, core: 2. Of those that a mesh axis runs over, the one named last changes fastest.
Arguments:
- x: bfloat16 [512, 2048], P('dp')
- lengths: int32 [512], P('dp')
- cache: bfloat16 [2, 512, 512, 576], P(None, 'dp')
- attn_norm: bfloat16 [2, 2048], replicated
- ffn_norm: bfloat16 [2, 2048], replicated
- wq: bfloat16 [2, 2048, 9216], P(None, None, 'tp')
- wo: bfloat16 [2, 8192, 2048], P(None, 'tp')
- w1: bfloat16 [2, 2048, 11264], P(None, None, ('dp', 'tp'))
- w3: bfloat16 [2, 2048, 11264], P(None, None, ('dp', 'tp'))
- w2: bfloat16 [2, 11264, 2048], P(None, ('dp', 'tp'))
Outputs:
- output: bfloat16 [512, 2048], P('dp')
All inputs are finite; a program needn't handle non-finite values.
Results may differ from the reference program's by a relative error of at most 0.02.
Values are sent between devices in bfloat16 or wider.
A program may use at most 1 GiB of HBM per device.

```python
import jax
import jax.numpy as jnp
from jax import lax

B = 512
S = 512
D = 2048
H = 16
F = 11264
LAYERS = 2
LAT = 512
ROPE = 64
KV = LAT + ROPE
EPS = 1e-6
SCALE = 192 ** -0.5


def setup_inputs(seed: int = 0) -> dict:
    ks = jax.random.split(jax.random.PRNGKey(seed), 10)

    def nrm(k, shape, std):
        return (jax.random.normal(k, shape, jnp.float32) * std).astype(jnp.bfloat16)

    def gain(k):
        return jax.random.uniform(k, (LAYERS, D), jnp.float32, 0.5, 1.5).astype(jnp.bfloat16)

    return {
        'x': nrm(ks[0], (B, D), 1.0),
        'lengths': jax.random.randint(ks[1], (B,), max(S // 8, 1), S + 1, jnp.int32),
        'cache': nrm(ks[2], (LAYERS, B, S, KV), 1.0),
        'attn_norm': gain(ks[3]),
        'ffn_norm': gain(ks[4]),
        'wq': nrm(ks[5], (LAYERS, D, H * KV), D ** -0.5),
        'wo': nrm(ks[6], (LAYERS, H * LAT, D), (H * LAT) ** -0.5 * S ** 0.5 / 8),
        'w1': nrm(ks[7], (LAYERS, D, F), D ** -0.5),
        'w3': nrm(ks[8], (LAYERS, D, F), D ** -0.5),
        'w2': nrm(ks[9], (LAYERS, F, D), 2.0 * F ** -0.5),
    }


def _rmsnorm(v, w):
    vf = v.astype(jnp.float32)
    r = lax.rsqrt(jnp.mean(vf * vf, axis=-1, keepdims=True) + EPS)
    return (vf * r * w.astype(jnp.float32)).astype(jnp.bfloat16)


def _attend(q, c, n):
    s = jnp.dot(q, c.T, preferred_element_type=jnp.float32) * SCALE
    s = jnp.where(jnp.arange(c.shape[0])[None, :] < n, s, -jnp.inf)
    p = jax.nn.softmax(s, axis=-1).astype(jnp.bfloat16)
    return jnp.dot(p, c[:, :LAT], preferred_element_type=jnp.float32).astype(jnp.bfloat16)


def _layer(x, lengths, c, an, fn, wq, wo, w1, w3, w2):
    nb = x.shape[0]
    h = _rmsnorm(x, an)
    q = jnp.dot(h, wq, preferred_element_type=jnp.float32).astype(jnp.bfloat16).reshape(nb, H, KV)
    o = lax.map(lambda t: _attend(*t), (q, c, lengths)).reshape(nb, H * LAT)
    x = x + jnp.dot(o, wo, preferred_element_type=jnp.float32).astype(jnp.bfloat16)
    g = _rmsnorm(x, fn)
    u = jnp.dot(g, w3, preferred_element_type=jnp.float32)
    v = jnp.dot(g, w1, preferred_element_type=jnp.float32)
    a = (jax.nn.silu(u) * v).astype(jnp.bfloat16)
    return x + jnp.dot(a, w2, preferred_element_type=jnp.float32).astype(jnp.bfloat16)


def reference(x, lengths, cache, attn_norm, ffn_norm, wq, wo, w1, w3, w2):
    def body(xc, lw):
        return _layer(xc, lengths, *lw), None
    out, _ = lax.scan(body, x, (cache, attn_norm, ffn_norm, wq, wo, w1, w3, w2))
    return out
```

```python
import functools

import jax
import jax.numpy as jnp
from jax import lax
from jax.experimental import pallas as pl
from jax.experimental.pallas import tpu as pltpu
from jax.sharding import PartitionSpec as P

LAT = 512
EPS = 1e-6
SCALE = 192 ** -0.5
BF = jnp.bfloat16
F32 = jnp.float32


def _rmsnorm(v, w):
    vf = v.astype(F32)
    r = lax.rsqrt(jnp.mean(vf * vf, axis=-1, keepdims=True) + EPS)
    return (vf * r * w.astype(F32)).astype(BF)


def _attn_kernel(layer, G, NS, order_ref, lens_ref, q_ref, ct_ref, o_ref, buf, sems):
    nb, nh, _ = q_ref.shape
    nmax = ct_ref.shape[3] // 128
    ng = nb // G

    def chunks(g):
        return lax.div(lens_ref[order_ref[g * G + G - 1]] + 127, 128)

    def copies(g, n):
        slot = lax.rem(g, NS)
        return [pltpu.make_async_copy(
            ct_ref.at[layer, order_ref[g * G + s], :, pl.ds(0, n * 128)],
            buf.at[slot, s, :, pl.ds(0, n * 128)],
            sems.at[slot, s]) for s in range(G)]

    def start(g):
        c = chunks(g)
        for n in range(1, nmax + 1):
            @pl.when(c == n)
            def _():
                for cp in copies(g, n):
                    cp.start()

    for g in range(NS - 1):
        start(g)

    def body(g, carry):
        @pl.when(g + NS - 1 < ng)
        def _():
            start(g + NS - 1)
        c = chunks(g)
        slot = lax.rem(g, NS)
        for n in range(1, nmax + 1):
            @pl.when(c == n)
            def _():
                N = n * 128
                for cp in copies(g, n):
                    cp.wait()
                bs = [order_ref[g * G + s] for s in range(G)]
                scs = [jnp.dot(q_ref[bs[s]], buf[slot, s, :, 0:N], preferred_element_type=F32)
                       for s in range(G)]
                pos = lax.broadcasted_iota(jnp.int32, (nh, N), 1)
                scs = [jnp.where(pos < lens_ref[bs[s]], scs[s] * SCALE, -jnp.inf) for s in range(G)]
                ms = [jnp.max(sc, axis=-1, keepdims=True) for sc in scs]
                es = [jnp.exp(sc - m) for sc, m in zip(scs, ms)]
                ds = [jnp.sum(e, axis=-1, keepdims=True) for e in es]
                ps = [(e / d).astype(BF) for e, d in zip(es, ds)]
                outs = [lax.dot_general(ps[s], buf[slot, s, 0:LAT, 0:N], (((1,), (1,)), ((), ())),
                                        preferred_element_type=F32) for s in range(G)]
                for s in range(G):
                    o_ref[bs[s]] = outs[s].astype(BF)
        return carry

    lax.fori_loop(0, ng, body, 0)


def _attention(layer, q, ct, order, lens, G=8, NS=3):
    nb, nh, kv = q.shape
    s_len = ct.shape[3]
    smem = pl.BlockSpec(memory_space=pltpu.SMEM)
    vmem = pl.BlockSpec(memory_space=pltpu.VMEM)
    return pl.pallas_call(
        functools.partial(_attn_kernel, layer, G, NS),
        out_shape=jax.ShapeDtypeStruct((nb, nh, LAT), BF),
        in_specs=[smem, smem, vmem, pl.BlockSpec(memory_space=pl.ANY)],
        out_specs=vmem,
        scratch_shapes=[pltpu.VMEM((NS, G, kv, s_len), BF), pltpu.SemaphoreType.DMA((NS, G))],
        compiler_params=pltpu.CompilerParams(vmem_limit_bytes=48 * 2 ** 20),
        name=f"attn{layer}",
    )(order, lens, q, ct)


def _sort_order(lens):
    i = jnp.arange(lens.shape[0])
    before = (lens[None, :] < lens[:, None]) | ((lens[None, :] == lens[:, None]) & (i[None, :] < i[:, None]))
    rank = jnp.sum(before.astype(jnp.int32), axis=1)
    return jnp.sum(jnp.where(rank[:, None] == i[None, :], i[:, None], 0), axis=0).astype(jnp.int32)


def solution(mesh):
    def body(x, lengths, cache, attn_norm, ffn_norm, wq, wo, w1, w3, w2):
        nb = x.shape[0]
        n_layers, _, s_len, kv = cache.shape
        nh = wq.shape[2] // kv
        ct = jnp.swapaxes(cache, 2, 3)
        order = _sort_order(lengths)
        for l in range(n_layers):
            h = _rmsnorm(x, attn_norm[l])
            q = jnp.dot(h, wq[l], preferred_element_type=F32).astype(BF).reshape(nb, nh, kv)
            o = _attention(l, q, ct, order, lengths).reshape(nb, nh * LAT)
            attn = lax.psum(jnp.dot(o, wo[l], preferred_element_type=F32), 'tp')
            x = x + attn.astype(BF)
            g = _rmsnorm(x, ffn_norm[l])
            gg = lax.all_gather(g, 'dp', axis=0, tiled=True)
            u = jnp.dot(gg, w3[l], preferred_element_type=F32)
            v = jnp.dot(gg, w1[l], preferred_element_type=F32)
            a = (jax.nn.silu(u) * v).astype(BF)
            yp = jnp.dot(a, w2[l], preferred_element_type=F32)
            y = lax.psum_scatter(yp, 'dp', scatter_dimension=0, tiled=True)
            y = lax.psum(y, 'tp')
            x = x + y.astype(BF)
        return x

    in_specs = (
        P('dp', None),
        P('dp'),
        P(None, 'dp', None, None),
        P(None, None),
        P(None, None),
        P(None, None, 'tp'),
        P(None, 'tp', None),
        P(None, None, ('dp', 'tp')),
        P(None, None, ('dp', 'tp')),
        P(None, ('dp', 'tp'), None),
    )
    return jax.shard_map(body, mesh=mesh, in_specs=in_specs, out_specs=P('dp', None), check_vma=False)
```

```python
import functools

import jax
import jax.numpy as jnp
from jax import lax
from jax.experimental import pallas as pl
from jax.experimental.pallas import tpu as pltpu
from jax.sharding import PartitionSpec as P

LAT = 512
EPS = 1e-6
SCALE = 192 ** -0.5
BF = jnp.bfloat16
F32 = jnp.float32
MESH = pl.DeviceIdType.MESH
VMEM = pl.BlockSpec(memory_space=pltpu.VMEM)
SMEM = pl.BlockSpec(memory_space=pltpu.SMEM)
ANY = pl.BlockSpec(memory_space=pl.ANY)


def _rmsnorm(v, w):
    vf = v.astype(F32)
    r = lax.rsqrt(jnp.mean(vf * vf, axis=-1, keepdims=True) + EPS)
    return (vf * r * w.astype(F32)).astype(BF)


def _attn_kernel(layer, G, NS, order_ref, lens_ref, base_ref, q_ref, ct_ref, wo_ref, out_ref,
                 buf, sems, wbuf, wsems, o_s, oflat):
    nh = q_ref.shape[1]
    nmax = ct_ref.shape[3] // 128
    nb = order_ref.shape[0]
    ng = nb // G
    wrows = wbuf.shape[0] // ng

    def chunks(g):
        return lax.div(lens_ref[order_ref[g * G + G - 1]] + 127, 128)

    def copies(g, n):
        slot = lax.rem(g, NS)
        return [pltpu.make_async_copy(
            ct_ref.at[layer, order_ref[g * G + s], :, pl.ds(0, n * 128)],
            buf.at[slot, s, :, pl.ds(0, n * 128)],
            sems.at[slot, s]) for s in range(G)]

    def wcopy(g):
        rows = pl.ds(pl.multiple_of(g * wrows, wrows), wrows)
        return pltpu.make_async_copy(wo_ref.at[layer, rows, :], wbuf.at[rows, :], wsems.at[g])

    def start(g):
        c = chunks(g)
        for n in range(1, nmax + 1):
            @pl.when(c == n)
            def _():
                for cp in copies(g, n):
                    cp.start()

    for g in range(NS - 1):
        start(g)

    def body(g, carry):
        @pl.when(g + NS - 1 < ng)
        def _():
            start(g + NS - 1)
        wcopy(g).start()
        c = chunks(g)
        slot = lax.rem(g, NS)
        for n in range(1, nmax + 1):
            @pl.when(c == n)
            def _():
                N = n * 128
                for cp in copies(g, n):
                    cp.wait()
                bs = [order_ref[g * G + s] for s in range(G)]
                scs = [jnp.dot(q_ref[bs[s]], buf[slot, s, :, 0:N], preferred_element_type=F32)
                       for s in range(G)]
                pos = lax.broadcasted_iota(jnp.int32, (nh, N), 1)
                scs = [jnp.where(pos < lens_ref[bs[s]], scs[s] * SCALE, -jnp.inf) for s in range(G)]
                ms = [jnp.max(sc, axis=-1, keepdims=True) for sc in scs]
                es = [jnp.exp(sc - m) for sc, m in zip(scs, ms)]
                ds = [jnp.sum(e, axis=-1, keepdims=True) for e in es]
                ps = [(e / d).astype(BF) for e, d in zip(es, ds)]
                outs = [lax.dot_general(ps[s], buf[slot, s, 0:LAT, 0:N], (((1,), (1,)), ((), ())),
                                        preferred_element_type=F32) for s in range(G)]
                for s in range(G):
                    row = pl.multiple_of((bs[s] - base_ref[0]) * nh, nh)
                    for i in range(LAT // 128):
                        o_s[pl.ds(row + i * nb * nh, nh), :] = outs[s][:, i * 128:(i + 1) * 128]
        return carry

    lax.fori_loop(0, ng, body, 0)
    for h in range(nh):
        for i in range(LAT // 128):
            c = h * LAT + i * 128
            oflat[:, c:c + 128] = o_s[pl.ds(i * nb * nh + h, nb, stride=nh), :].astype(BF)
    for g in range(ng):
        wcopy(g).wait()
    nblk = 512

    def mm(j, carry):
        cols = pl.ds(pl.multiple_of(j * nblk, nblk), nblk)
        out_ref[:, cols] = jnp.dot(oflat[...], wbuf[:, cols], preferred_element_type=F32)
        return carry
    lax.fori_loop(0, out_ref.shape[1] // nblk, mm, 0)


def _attention(layer, q, ct, order, base, lens, wo, G=8, NS=3):
    _, nh, kv = q.shape
    nb = order.shape[0]
    s_len = ct.shape[3]
    hid, d = wo.shape[1], wo.shape[2]
    return pl.pallas_call(
        functools.partial(_attn_kernel, layer, G, NS),
        out_shape=jax.ShapeDtypeStruct((nb, d), F32),
        in_specs=[SMEM, SMEM, SMEM, VMEM, ANY, ANY],
        out_specs=VMEM,
        scratch_shapes=[
            pltpu.VMEM((NS, G, kv, s_len), BF), pltpu.SemaphoreType.DMA((NS, G)),
            pltpu.VMEM((hid, d), BF), pltpu.SemaphoreType.DMA((nb // G,)),
            pltpu.VMEM((LAT // 128 * nb * nh, 128), F32), pltpu.VMEM((nb, hid), BF),
        ],
        compiler_params=pltpu.CompilerParams(vmem_limit_bytes=48 * 2 ** 20),
        cost_estimate=pl.CostEstimate(flops=20 * 10 ** 9, bytes_accessed=40 * 2 ** 20, transcendentals=0),
        name=f"attn{layer}",
    )(order, lens, base, q, ct, wo)


def _sort_order(lens):
    i = jnp.arange(lens.shape[0])
    before = (lens[None, :] < lens[:, None]) | ((lens[None, :] == lens[:, None]) & (i[None, :] < i[:, None]))
    rank = jnp.sum(before.astype(jnp.int32), axis=1)
    return jnp.sum(jnp.where(rank[:, None] == i[None, :], i[:, None], 0), axis=0).astype(jnp.int32)


XLOC = {1: (1, 0), 0: (2, 0)}
YLOC = {0: (1, 1), 1: (2, 1)}


def _ffn_kernel(layer, last, CA, xo_ref, pa_ref, pb_ref, fn_ref, an_ref, w1_ref, w3_ref, w2_ref, wq_ref, *rest):
    if last:
        out_ref, rest = rest[0], rest[1:]
    else:
        xn_ref, q_ref, rest = rest[0], rest[1], rest[2:]
    (w13, w2v, wqv, gbuf, ybuf, sbuf, abuf, xp, xall,
     r1x_own, r1x_y, r1y_own, r1y_x, r2x, r2y,
     wsem, w2sem, wqsem, ss, rs) = rest
    tp = lax.axis_index("tp")
    dp = lax.axis_index("dp")
    xi, ci = lax.div(dp, 2), lax.rem(dp, 2)
    SIB = (tp, xi * 2 + 1 - ci)
    X = (tp, (1 - xi) * 2 + ci)
    Y = (1 - tp, dp)

    bar = pltpu.get_barrier_semaphore()
    for peer in (SIB, X, Y):
        pl.semaphore_signal(bar, inc=1, device_id=peer, device_id_type=MESH)

    nblk = w1_ref.shape[2] // 128
    wcopies = []
    for j in range(nblk):
        for i, w in enumerate((w3_ref, w1_ref)):
            wcopies.append(pltpu.make_async_copy(
                w.at[layer, :, pl.ds(j * 128, 128)], w13.at[:, pl.ds(j * 256 + i * 128, 128)],
                wsem.at[j, i]))
    w2copy = pltpu.make_async_copy(w2_ref.at[layer], w2v, w2sem)
    for cp in wcopies:
        cp.start()
    w2copy.start()
    wqcopies = []
    if not last:
        nq = wqsem.shape[0]
        qc = wqv.shape[1] // nq
        for j in range(nq):
            cols = pl.ds(j * qc, qc)
            wqcopies.append(pltpu.make_async_copy(wq_ref.at[layer + 1, :, cols], wqv.at[:, cols], wqsem.at[j]))
        for cp in wqcopies:
            cp.start()

    count = [0]

    def remote(src, dst, dev):
        i = count[0]
        count[0] += 1
        return pltpu.make_async_remote_copy(src_ref=src, dst_ref=dst, send_sem=ss.at[i], recv_sem=rs.at[i],
                                            device_id=dev, device_id_type=MESH)

    colA, colB = pl.ds(0, CA), pl.ds(CA, gbuf.shape[-1] - CA)
    own_sib = remote(gbuf.at[0, 0], gbuf.at[0, 1], SIB)
    own_x = {p: remote(gbuf.at[0, 0, p], gbuf.at[XLOC[p][0], 0, XLOC[p][1]], X) for p in (1, 0)}
    own_y = {p: remote(gbuf.at[0, 0, p], gbuf.at[YLOC[p][0], 0, YLOC[p][1]], Y) for p in (0, 1)}
    relay_x = remote(gbuf.at[1, 0, 1], gbuf.at[3, 0, 0], X)
    relay_y = remote(gbuf.at[1, 0, 0], gbuf.at[3, 0, 1], Y)
    sib_g = {k: remote(gbuf.at[k, 0], gbuf.at[k, 1], SIB) for k in (1, 2, 3)}
    sib_y = {k: remote(ybuf.at[k, 1], sbuf.at[k], SIB) for k in range(4)}
    st1_x = {p: remote(ybuf.at[XLOC[p][0], 0, XLOC[p][1], :, colA], r1x_own.at[p], X) for p in (0, 1)}
    st1_y = {p: remote(ybuf.at[YLOC[p][0], 0, YLOC[p][1], :, colB], r1y_own.at[p], Y) for p in (0, 1)}
    st1_dx = {p: remote(ybuf.at[3, 0, p, :, colA], r1x_y.at[p], X) for p in (0, 1)}
    st1_dy = {p: remote(ybuf.at[3, 0, p, :, colB], r1y_x.at[p], Y) for p in (0, 1)}
    st2_y = {p: remote(r1x_y.at[p], r2y.at[p], Y) for p in (0, 1)}
    st2_x = {p: remote(r1y_x.at[p], r2x.at[p], X) for p in (0, 1)}
    mine = [pl.ds(pl.multiple_of(tp * 64 + p * 32, 32), 32) for p in (0, 1)]
    xg = {p: remote(xall.at[mine[p]], xall.at[mine[p]], Y) for p in (0, 1)}

    x1 = xo_ref[...].astype(F32) + (pa_ref[...] + pb_ref[...]).astype(BF).astype(F32)
    x1 = x1.astype(BF)
    xp[...] = x1
    gbuf[0, 0] = _rmsnorm(x1, fn_ref[layer:layer + 1, :]).reshape(2, 32, -1)

    pl.semaphore_wait(bar, 3)
    own_sib.start()
    own_x[1].start()
    own_y[0].start()
    own_x[0].start()
    own_y[1].start()

    def combine(k):
        sib_y[k].wait_recv()
        ybuf[k, 0] = ybuf[k, 0] + sbuf[k]

    def chunk(k, carry):
        @pl.when(k == 0)
        def _():
            own_sib.wait_recv()
            for cp in wcopies:
                cp.wait()
        for kk in (1, 2, 3):
            @pl.when(k == kk)
            def _():
                sib_g[kk].wait_recv()
        g = gbuf[k].reshape(128, -1)
        for j in range(nblk):
            uv = jnp.dot(g, w13[:, j * 256:(j + 1) * 256], preferred_element_type=F32)
            u, v = uv[:, :128], uv[:, 128:]
            abuf[:, j * 128:(j + 1) * 128] = (jax.nn.silu(u) * v).astype(BF)

        @pl.when(k == 0)
        def _():
            own_x[1].wait_recv()
            own_y[0].wait_recv()
            relay_x.start()
            relay_y.start()
            sib_g[1].start()
            w2copy.wait()

        @pl.when(k == 1)
        def _():
            own_x[0].wait_recv()
            own_y[1].wait_recv()
            sib_g[2].start()
            combine(0)

        @pl.when(k == 2)
        def _():
            relay_x.wait_recv()
            relay_y.wait_recv()
            sib_g[3].start()
            combine(1)
            st1_x[1].start()
            st1_y[0].start()

        @pl.when(k == 3)
        def _():
            combine(2)
            st1_x[0].start()
            st1_y[1].start()

        a = abuf[...]
        nn = 512
        for j in range(ybuf.shape[-1] // nn):
            y = jnp.dot(a, w2v[:, j * nn:(j + 1) * nn], preferred_element_type=F32)
            ybuf[k, :, :, :, j * nn:(j + 1) * nn] = y.reshape(2, 2, 32, nn)
        for kk in range(4):
            @pl.when(k == kk)
            def _():
                sib_y[kk].start()
        return carry

    lax.fori_loop(0, 4, chunk, 0)
    sib_y[3].wait_recv()
    for p in (0, 1):
        ybuf[3, 0, p] = ybuf[3, 0, p] + sbuf[3, p]
        st1_dx[p].start()
        st1_dy[p].start()
    for p in (0, 1):
        st1_dx[p].wait_recv()
        k, j = YLOC[p]
        r1x_y[p] = r1x_y[p] + ybuf[k, 0, j, :, 0:CA]
        st2_y[p].start()
        st1_dy[p].wait_recv()
        k, j = XLOC[p]
        r1y_x[p] = r1y_x[p] + ybuf[k, 0, j, :, CA:]
        st2_x[p].start()
    for p in (0, 1):
        st1_x[p].wait_recv()
        st1_y[p].wait_recv()
        st2_y[p].wait_recv()
        st2_x[p].wait_recv()
        ya = ybuf[0, 0, p, :, 0:CA] + r1x_own[p] + r2y[p]
        yb = ybuf[0, 0, p, :, CA:] + r1y_own[p] + r2x[p]
        xv = xp[p * 32:(p + 1) * 32, :].astype(F32)
        y = jnp.concatenate([ya, yb], axis=-1).astype(BF).astype(F32)
        xn = (xv + y).astype(BF)
        xall[mine[p], :] = xn
        if not last:
            xn_ref[p * 32:(p + 1) * 32, :] = xn
        xg[p].start()
    for p in (0, 1):
        xg[p].wait_recv()
    if last:
        out_ref[...] = xall[...]
    else:
        h = _rmsnorm(xall[...], an_ref[layer + 1:layer + 2, :])
        for j, cp in enumerate(wqcopies):
            cp.wait()
            cols = pl.ds(j * qc, qc)
            q_ref[:, cols] = jnp.dot(h, wqv[:, cols], preferred_element_type=F32).astype(BF)
    for cp in [own_sib, relay_x, relay_y, *own_x.values(), *own_y.values(), *sib_g.values(), *sib_y.values(),
               *st1_x.values(), *st1_y.values(), *st1_dx.values(), *st1_dy.values(),
               *st2_x.values(), *st2_y.values(), *xg.values()]:
        cp.wait_send()


NCOPY = 31


def _ffn(layer, last, xo, pa, pb, fn, an, w1, w3, w2, wq, CA=1024):
    rows, d = xo.shape
    f = w1.shape[2]
    nq = wq.shape[2]
    nqs = 4
    if last:
        out_shape = [jax.ShapeDtypeStruct((2 * rows, d), BF)]
    else:
        out_shape = [jax.ShapeDtypeStruct((rows, d), BF), jax.ShapeDtypeStruct((2 * rows, nq), BF)]
    CB = d - CA
    scratch = [
        pltpu.VMEM((d, 2 * f), BF), pltpu.VMEM((f, d), BF),
        pltpu.VMEM((8, 128) if last else (d, nq), BF),
        pltpu.VMEM((4, 2, 2, 32, d), BF), pltpu.VMEM((4, 2, 2, 32, d), F32), pltpu.VMEM((4, 2, 32, d), F32),
        pltpu.VMEM((128, f), BF), pltpu.VMEM((rows, d), BF), pltpu.VMEM((2 * rows, d), BF),
        pltpu.VMEM((2, 32, CA), F32), pltpu.VMEM((2, 32, CA), F32),
        pltpu.VMEM((2, 32, CB), F32), pltpu.VMEM((2, 32, CB), F32),
        pltpu.VMEM((2, 32, CB), F32), pltpu.VMEM((2, 32, CA), F32),
        pltpu.SemaphoreType.DMA((f // 128, 2)), pltpu.SemaphoreType.DMA, pltpu.SemaphoreType.DMA((nqs,)),
        pltpu.SemaphoreType.DMA((NCOPY,)), pltpu.SemaphoreType.DMA((NCOPY,)),
    ]
    return pl.pallas_call(
        functools.partial(_ffn_kernel, layer, last, CA),
        out_shape=out_shape,
        in_specs=[VMEM, VMEM, VMEM, VMEM, VMEM, ANY, ANY, ANY, ANY],
        out_specs=[VMEM] * len(out_shape),
        scratch_shapes=scratch,
        compiler_params=pltpu.CompilerParams(collective_id=layer, has_side_effects=True,
                                             vmem_limit_bytes=62 * 2 ** 20),
        name=f"ffn{layer}",
    )(xo, pa, pb, fn, an, w1, w3, w2, wq)


def solution(mesh):
    def body(x, lengths, cache, attn_norm, ffn_norm, wq, wo, w1, w3, w2):
        nb = x.shape[0]
        n_layers, _, s_len, kv = cache.shape
        nh = wq.shape[2] // kv
        half = nb // 2
        tp = lax.axis_index('tp')
        ct = jnp.swapaxes(cache, 2, 3)
        ord0 = _sort_order(lengths[:half])
        ord1 = _sort_order(lengths[half:]) + half
        first = jnp.where(tp == 0, ord1, ord0)
        second = jnp.where(tp == 0, ord0, ord1)
        base1 = jnp.reshape((1 - tp) * half, (1,)).astype(jnp.int32)
        base2 = jnp.reshape(tp * half, (1,)).astype(jnp.int32)
        xo = lax.dynamic_slice_in_dim(x, tp * half, half, 0)
        h = _rmsnorm(x, attn_norm[0])
        q = jnp.dot(h, wq[0], preferred_element_type=F32).astype(BF)
        for l in range(n_layers):
            last = l == n_layers - 1
            q3 = q.reshape(nb, nh, kv)
            pa = _attention(l, q3, ct, first, base1, lengths, wo)
            pa = lax.ppermute(pa, 'tp', [(0, 1), (1, 0)])
            pb = _attention(l, q3, ct, second, base2, lengths, wo)
            res = _ffn(l, last, xo, pb, pa, ffn_norm, attn_norm, w1, w3, w2, wq)
            if last:
                return res[0]
            xo, q = res

    in_specs = (
        P('dp', None),
        P('dp'),
        P(None, 'dp', None, None),
        P(None, None),
        P(None, None),
        P(None, None, 'tp'),
        P(None, 'tp', None),
        P(None, None, ('dp', 'tp')),
        P(None, None, ('dp', 'tp')),
        P(None, ('dp', 'tp'), None),
    )
    return jax.shard_map(body, mesh=mesh, in_specs=in_specs, out_specs=P('dp', None), check_vma=False)
```

```python
import functools

import jax
import jax.numpy as jnp
from jax import lax
from jax.experimental import pallas as pl
from jax.experimental.pallas import tpu as pltpu
from jax.sharding import PartitionSpec as P

LAT = 512
EPS = 1e-6
SCALE = 192 ** -0.5
BF = jnp.bfloat16
F32 = jnp.float32
MESH = pl.DeviceIdType.MESH
VMEM = pl.BlockSpec(memory_space=pltpu.VMEM)
SMEM = pl.BlockSpec(memory_space=pltpu.SMEM)
ANY = pl.BlockSpec(memory_space=pl.ANY)


def _rmsnorm(v, w):
    vf = v.astype(F32)
    r = lax.rsqrt(jnp.mean(vf * vf, axis=-1, keepdims=True) + EPS)
    return (vf * r * w.astype(F32)).astype(BF)


def _project(h, w, j, q_ref, nb, nh, kv):
    nblk = -(-kv // 128)
    val = jnp.dot(h, w, preferred_element_type=F32).astype(BF).astype(F32)
    lo = (kv // 128) * 128
    odd = pltpu.roll(val[:, lo:lo + nblk * 128], nblk * 128 - (kv - lo), 1)
    for t, v in ((0, val), (1, odd)):
        for i in range(nblk):
            q_ref[pl.ds(i * nb * nh + 2 * j + t, nb, stride=nh), :] = v[:, i * 128:(i + 1) * 128]


def _first_kernel(lens_ref, x_ref, an_ref, wq_ref, order_ref, q_ref, wbuf, wsem):
    nb = x_ref.shape[0]
    kv2 = wbuf.shape[2]
    nj = wbuf.shape[0]
    cps = [pltpu.make_async_copy(wq_ref.at[0, :, pl.ds(j * kv2, kv2)], wbuf.at[j], wsem.at[j]) for j in range(nj)]
    for cp in cps:
        cp.start()
    tp = lax.axis_index("tp").astype(F32)
    half = nb // 2
    r = lax.broadcasted_iota(jnp.int32, (nb, nb), 0).astype(F32)
    c = lax.broadcasted_iota(jnp.int32, (nb, nb), 1).astype(F32)
    rh = (r >= half).astype(F32)
    ch = (c >= half).astype(F32)
    key = jnp.broadcast_to(lens_ref[...].astype(F32), (nb, nb)) * nb + c
    mine = jnp.sum(jnp.where(r == c, key, 0.0), axis=1, keepdims=True)
    rank = jnp.sum(jnp.where((rh == ch) & (key < mine), 1.0, 0.0), axis=1, keepdims=True)
    want = jnp.where(ch == 0.0, 1.0 - tp, tp)
    hit = (rank == c - ch * half) & (rh == want)
    order_ref[...] = jnp.sum(jnp.where(hit, r, 0.0), axis=0, keepdims=True).astype(jnp.int32)
    h = _rmsnorm(x_ref[...], an_ref[0:1, :])
    for j in range(nj):
        cps[j].wait()
        _project(h, wbuf[j], j, q_ref, nb, 2 * nj, kv2 // 2)


def _first(lens, x, an, wq, nh):
    nb, d = x.shape
    kv = wq.shape[2] // nh
    return pl.pallas_call(
        _first_kernel,
        out_shape=[jax.ShapeDtypeStruct((1, nb), jnp.int32),
                   jax.ShapeDtypeStruct((-(-kv // 128) * nb * nh, 128), F32)],
        in_specs=[VMEM, VMEM, VMEM, ANY],
        out_specs=[VMEM, VMEM],
        scratch_shapes=[pltpu.VMEM((nh // 2, d, 2 * kv), BF), pltpu.SemaphoreType.DMA((nh // 2,))],
        compiler_params=pltpu.CompilerParams(vmem_limit_bytes=32 * 2 ** 20),
        name="first",
    )(lens.reshape(1, nb), x, an, wq)


def _attn_kernel(layer, off, nh, G, NS, order_ref, lens_ref, q_ref, ct_ref, wo_ref, out_ref,
                 buf, sems, wbuf, wsems, o_s, oflat):
    kv = ct_ref.shape[2]
    nmax = ct_ref.shape[3] // 128
    nb = out_ref.shape[0]
    nall = ct_ref.shape[1]
    ng = nb // G
    wrows = wbuf.shape[0] // ng
    qblk = -(-kv // 128)

    def seq(i):
        return order_ref[0, off + i]

    def chunks(g):
        return lax.div(lens_ref[seq(g * G + G - 1)] + 127, 128)

    def copies(g, n):
        slot = lax.rem(g, NS)
        return [pltpu.make_async_copy(
            ct_ref.at[layer, seq(g * G + s), :, pl.ds(0, n * 128)],
            buf.at[slot, s, :, pl.ds(0, n * 128)],
            sems.at[slot, s]) for s in range(G)]

    def wcopy(g):
        rows = pl.ds(pl.multiple_of(g * wrows, wrows), wrows)
        return pltpu.make_async_copy(wo_ref.at[layer, rows, :], wbuf.at[rows, :], wsems.at[g])

    def start(g):
        c = chunks(g)
        for n in range(1, nmax + 1):
            @pl.when(c == n)
            def _():
                for cp in copies(g, n):
                    cp.start()

    def qrow(b):
        parts = [q_ref[pl.ds(pl.multiple_of(i * nall * nh + b * nh, nh), nh), :] for i in range(qblk)]
        return jnp.concatenate(parts, axis=-1)[:, :kv].astype(BF)

    for g in range(NS - 1):
        start(g)

    def body(g, carry):
        @pl.when(g + NS - 1 < ng)
        def _():
            start(g + NS - 1)
        wcopy(g).start()
        c = chunks(g)
        slot = lax.rem(g, NS)
        for n in range(1, nmax + 1):
            @pl.when(c == n)
            def _():
                N = n * 128
                for cp in copies(g, n):
                    cp.wait()
                bs = [seq(g * G + s) for s in range(G)]
                scs = [jnp.dot(qrow(bs[s]), buf[slot, s, :, 0:N], preferred_element_type=F32)
                       for s in range(G)]
                pos = lax.broadcasted_iota(jnp.int32, (nh, N), 1)
                scs = [jnp.where(pos < lens_ref[bs[s]], scs[s] * SCALE, -jnp.inf) for s in range(G)]
                ms = [jnp.max(sc, axis=-1, keepdims=True) for sc in scs]
                es = [jnp.exp(sc - m) for sc, m in zip(scs, ms)]
                ds = [jnp.sum(e, axis=-1, keepdims=True) for e in es]
                ps = [(e / d).astype(BF) for e, d in zip(es, ds)]
                outs = [lax.dot_general(ps[s], buf[slot, s, 0:LAT, 0:N], (((1,), (1,)), ((), ())),
                                        preferred_element_type=F32) for s in range(G)]
                for s in range(G):
                    row = lax.rem(bs[s], nb) * nh
                    for i in range(LAT // 128):
                        o_s[pl.ds(pl.multiple_of(row + i * nb * nh, nh), nh), :] = outs[s][:, i * 128:(i + 1) * 128]
        return carry

    lax.fori_loop(0, ng, body, 0)
    for h in range(nh):
        for i in range(LAT // 128):
            c = h * LAT + i * 128
            oflat[:, c:c + 128] = o_s[pl.ds(i * nb * nh + h, nb, stride=nh), :].astype(BF)
    for g in range(ng):
        wcopy(g).wait()
    nblk = 1024

    def mm(j, carry):
        cols = pl.ds(pl.multiple_of(j * nblk, nblk), nblk)
        out_ref[:, cols] = jnp.dot(oflat[...], wbuf[:, cols], preferred_element_type=F32)
        return carry
    lax.fori_loop(0, out_ref.shape[1] // nblk, mm, 0)


def _attention(layer, off, q, ct, order, lens, wo, nh, G=8, NS=3):
    kv, s_len = ct.shape[2:]
    nb = order.shape[1] // 2
    hid, d = wo.shape[1], wo.shape[2]
    return pl.pallas_call(
        functools.partial(_attn_kernel, layer, off, nh, G, NS),
        out_shape=jax.ShapeDtypeStruct((nb, d), F32),
        in_specs=[SMEM, SMEM, VMEM, ANY, ANY],
        out_specs=VMEM,
        scratch_shapes=[
            pltpu.VMEM((NS, G, kv, s_len), BF), pltpu.SemaphoreType.DMA((NS, G)),
            pltpu.VMEM((hid, d), BF), pltpu.SemaphoreType.DMA((nb // G,)),
            pltpu.VMEM((LAT // 128 * nb * nh, 128), F32), pltpu.VMEM((nb, hid), BF),
        ],
        compiler_params=pltpu.CompilerParams(vmem_limit_bytes=40 * 2 ** 20),
        cost_estimate=pl.CostEstimate(flops=20 * 10 ** 9, bytes_accessed=40 * 2 ** 20, transcendentals=0),
        name=f"attn{layer}",
    )(order, lens, q, ct, wo)


XLOC = {1: (1, 0), 0: (2, 0)}
YLOC = {0: (1, 1), 1: (2, 1)}
W = 512
A = (0, 1)
B = (2, 3)
QORDER = (0, 2, 1, 3)
HALF = 64


def _ffn_kernel(layer, last, nh, xo_ref, pa_ref, pb_ref, fn_ref, an_ref, w1_ref, w3_ref, w2_ref, wq_ref, *rest):
    if last:
        out_ref, rest = rest[0], rest[1:]
    else:
        xn_ref, q_ref, rest = rest[0], rest[1], rest[2:]
    (w13, w2v, wqv, gbuf, ybuf, sbuf, abuf, xp, xall,
     r1x_own, r1x_y, r1y_own, r1y_x, r2x, r2y,
     wsem, w2sem, wqsem, ss, rs) = rest
    tp = lax.axis_index("tp")
    dp = lax.axis_index("dp")
    xi, ci = lax.div(dp, 2), lax.rem(dp, 2)
    SIB = (tp, xi * 2 + 1 - ci)
    X = (tp, (1 - xi) * 2 + ci)
    Y = (1 - tp, dp)

    bar = pltpu.get_barrier_semaphore()
    for peer in (SIB, X, Y):
        pl.semaphore_signal(bar, inc=1, device_id=peer, device_id_type=MESH)

    nblk = w1_ref.shape[2] // 128
    wcopies = []
    for j in range(nblk):
        for i, w in enumerate((w3_ref, w1_ref)):
            wcopies.append(pltpu.make_async_copy(
                w.at[layer, :, pl.ds(j * 128, 128)], w13.at[:, pl.ds(j * 256 + i * 128, 128)],
                wsem.at[j, i]))
    w2copy = pltpu.make_async_copy(w2_ref.at[layer], w2v, w2sem)
    for cp in wcopies:
        cp.start()
    w2copy.start()
    nj = nh // 2
    if not last:
        kv2 = wq_ref.shape[2] // nj
        dst = [w13.at[:, pl.ds(j * kv2, kv2)] if j < 2 else wqv.at[j - 2] for j in range(nj)]
        wqcopies = [pltpu.make_async_copy(wq_ref.at[layer + 1, :, pl.ds(j * kv2, kv2)], dst[j], wqsem.at[j])
                    for j in range(nj)]
        for cp in wqcopies[2:]:
            cp.start()

    count = [16]

    def remote(src, dst, dev, i=None):
        if i is None:
            i = count[0]
            count[0] += 1
        return pltpu.make_async_remote_copy(src_ref=src, dst_ref=dst, send_sem=ss.at[i], recv_sem=rs.at[i],
                                            device_id=dev, device_id_type=MESH)

    def cols(q):
        return pl.ds(q * W, W)

    colA, colB = pl.ds(A[0] * W, len(A) * W), pl.ds(B[0] * W, len(B) * W)
    own_sib = remote(gbuf.at[0, 0], gbuf.at[0, 1], SIB)
    own_x = {p: remote(gbuf.at[0, 0, p], gbuf.at[XLOC[p][0], 0, XLOC[p][1]], X) for p in (1, 0)}
    own_y = {p: remote(gbuf.at[0, 0, p], gbuf.at[YLOC[p][0], 0, YLOC[p][1]], Y) for p in (0, 1)}
    relay_x = remote(gbuf.at[1, 0, 1], gbuf.at[3, 0, 0], X)
    relay_y = remote(gbuf.at[1, 0, 0], gbuf.at[3, 0, 1], Y)
    sib_g = {k: remote(gbuf.at[k, 0], gbuf.at[k, 1], SIB) for k in (1, 2, 3)}
    PS = (0, 1)
    st1_x = {p: remote(ybuf.at[XLOC[p][0], 0, XLOC[p][1], :, colA], r1x_own.at[p], X) for p in PS}
    st1_y = {p: remote(ybuf.at[YLOC[p][0], 0, YLOC[p][1], :, colB], r1y_own.at[p], Y) for p in PS}
    st1_dx = {(p, q): remote(ybuf.at[3, 0, p, :, cols(q)], r1x_y.at[p, i], X) for p in PS for i, q in enumerate(A)}
    st1_dy = {(p, q): remote(ybuf.at[3, 0, p, :, cols(q)], r1y_x.at[p, i], Y) for p in PS for i, q in enumerate(B)}
    st2_y = {(p, q): remote(r1x_y.at[p, i], r2y.at[p, i], Y) for p in PS for i, q in enumerate(A)}
    st2_x = {(p, q): remote(r1y_x.at[p, i], r2x.at[p, i], X) for p in PS for i, q in enumerate(B)}
    mine = [pl.ds(pl.multiple_of(tp * HALF + p * 32, 32), 32) for p in PS]
    xg = {(p, q): remote(xall.at[mine[p], cols(q)], xall.at[mine[p], cols(q)], Y) for p in PS for q in A + B}

    def sib_y(k, q):
        return remote(ybuf.at[k, 1, :, :, cols(q)], sbuf.at[k, :, :, cols(q)], SIB, k * 4 + q)

    if xo_ref.shape[0] == HALF:
        xo = xo_ref[...]
    else:
        xo = xo_ref[pl.ds(pl.multiple_of(tp * HALF, HALF), HALF), :]
    x1 = (xo.astype(F32) + (pa_ref[...] + pb_ref[...]).astype(BF).astype(F32)).astype(BF)
    xp[...] = x1
    gbuf[0, 0] = _rmsnorm(x1, fn_ref[layer:layer + 1, :]).reshape(2, 32, -1)

    pl.semaphore_wait(bar, 3)
    own_sib.start()
    own_x[1].start()
    own_y[0].start()
    own_x[0].start()
    own_y[1].start()

    def combine(k, q):
        sib_y(k, q).wait_recv()
        ybuf[k, 0, :, :, cols(q)] = ybuf[k, 0, :, :, cols(q)] + sbuf[k, :, :, cols(q)]

    def chunk(k, carry):
        @pl.when(k == 0)
        def _():
            own_sib.wait_recv()
            for cp in wcopies:
                cp.wait()
        for kk in (1, 2, 3):
            @pl.when(k == kk)
            def _():
                sib_g[kk].wait_recv()
        g = gbuf[k].reshape(2 * HALF, -1)
        for j in range(nblk):
            uv = jnp.dot(g, w13[:, j * 256:(j + 1) * 256], preferred_element_type=F32)
            u, v = uv[:, :128], uv[:, 128:]
            abuf[:, j * 128:(j + 1) * 128] = (jax.nn.silu(u) * v).astype(BF)

        @pl.when(k == 0)
        def _():
            own_x[1].wait_recv()
            own_y[0].wait_recv()
            relay_x.start()
            relay_y.start()
            sib_g[1].start()
            w2copy.wait()

        @pl.when(k == 1)
        def _():
            own_x[0].wait_recv()
            own_y[1].wait_recv()
            sib_g[2].start()
            for q in QORDER:
                combine(0, q)

        @pl.when(k == 2)
        def _():
            relay_x.wait_recv()
            relay_y.wait_recv()
            sib_g[3].start()
            for q in QORDER:
                combine(1, q)
            st1_x[1].start()
            st1_y[0].start()

        @pl.when(k == 3)
        def _():
            if not last:
                for cp in wqcopies[:2]:
                    cp.start()
            for q in QORDER:
                combine(2, q)
            st1_x[0].start()
            st1_y[1].start()

        a = abuf[...]
        for q in QORDER:
            y = jnp.dot(a, w2v[:, q * W:(q + 1) * W], preferred_element_type=F32)
            ybuf[k, :, :, :, q * W:(q + 1) * W] = y.reshape(2, 2, 32, W)
            sib_y(k, q).start()
        return carry

    lax.fori_loop(0, 4, chunk, 0)
    for q in QORDER:
        combine(3, q)
        for p in PS:
            (st1_dx if q in A else st1_dy)[p, q].start()
    for q in QORDER:
        for p in PS:
            if q in A:
                st1_dx[p, q].wait_recv()
                (k, j), i = YLOC[p], A.index(q)
                r1x_y[p, i] = r1x_y[p, i] + ybuf[k, 0, j, :, q * W:(q + 1) * W]
                st2_y[p, q].start()
            else:
                st1_dy[p, q].wait_recv()
                (k, j), i = XLOC[p], B.index(q)
                r1y_x[p, i] = r1y_x[p, i] + ybuf[k, 0, j, :, q * W:(q + 1) * W]
                st2_x[p, q].start()
    for p in PS:
        st1_x[p].wait_recv()
        st1_y[p].wait_recv()
    for q in QORDER:
        for p in PS:
            c = slice(q * W, (q + 1) * W)
            y = ybuf[0, 0, p, :, c]
            if q in A:
                st2_y[p, q].wait_recv()
                i = A.index(q)
                y = y + r1x_own[p, :, i * W:(i + 1) * W] + r2y[p, i]
            else:
                st2_x[p, q].wait_recv()
                i = B.index(q)
                y = y + r1y_own[p, :, i * W:(i + 1) * W] + r2x[p, i]
            xn = (xp[p * 32:(p + 1) * 32, c].astype(F32) + y.astype(BF).astype(F32)).astype(BF)
            xall[mine[p], c] = xn
            if not last:
                xn_ref[p * 32:(p + 1) * 32, c] = xn
            xg[p, q].start()
    for cp in xg.values():
        cp.wait_recv()
    if last:
        out_ref[...] = xall[...]
    else:
        h = _rmsnorm(xall[...], an_ref[layer + 1:layer + 2, :])
        for j, cp in enumerate(wqcopies):
            cp.wait()
            _project(h, dst[j][...], j, q_ref, 2 * HALF, nh, kv2 // 2)
    for cp in [own_sib, relay_x, relay_y, *own_x.values(), *own_y.values(), *sib_g.values(),
               *st1_x.values(), *st1_y.values(), *st1_dx.values(), *st1_dy.values(),
               *st2_x.values(), *st2_y.values(), *xg.values()]:
        cp.wait_send()
    for k in range(4):
        for q in QORDER:
            sib_y(k, q).wait_send()


NCOPY = 16 + 10 + 4 + 8 + 8 + 8


def _ffn(layer, last, nh, xo, pa, pb, fn, an, w1, w3, w2, wq):
    rows, d = pa.shape
    f = w1.shape[2]
    kv = wq.shape[2] // nh
    if last:
        out_shape = [jax.ShapeDtypeStruct((2 * rows, d), BF)]
    else:
        out_shape = [jax.ShapeDtypeStruct((rows, d), BF),
                     jax.ShapeDtypeStruct((-(-kv // 128) * 2 * rows * nh, 128), F32)]
    NA, NB = len(A), len(B)
    scratch = [
        pltpu.VMEM((d, 2 * f), BF), pltpu.VMEM((f, d), BF),
        pltpu.VMEM((1, 16, 128) if last else (nh // 2 - 2, d, 2 * kv), BF),
        pltpu.VMEM((4, 2, 2, 32, d), BF), pltpu.VMEM((4, 2, 2, 32, d), F32), pltpu.VMEM((4, 2, 32, d), F32),
        pltpu.VMEM((128, f), BF), pltpu.VMEM((rows, d), BF), pltpu.VMEM((2 * rows, d), BF),
        pltpu.VMEM((2, 32, NA * W), F32), pltpu.VMEM((2, NA, 32, W), F32),
        pltpu.VMEM((2, 32, NB * W), F32), pltpu.VMEM((2, NB, 32, W), F32),
        pltpu.VMEM((2, NB, 32, W), F32), pltpu.VMEM((2, NA, 32, W), F32),
        pltpu.SemaphoreType.DMA((f // 128, 2)), pltpu.SemaphoreType.DMA, pltpu.SemaphoreType.DMA((nh // 2,)),
        pltpu.SemaphoreType.DMA((NCOPY,)), pltpu.SemaphoreType.DMA((NCOPY,)),
    ]
    return pl.pallas_call(
        functools.partial(_ffn_kernel, layer, last, nh),
        out_shape=out_shape,
        in_specs=[VMEM, VMEM, VMEM, VMEM, VMEM, ANY, ANY, ANY, ANY],
        out_specs=[VMEM] * len(out_shape),
        scratch_shapes=scratch,
        compiler_params=pltpu.CompilerParams(collective_id=layer, has_side_effects=True,
                                             vmem_limit_bytes=46 * 2 ** 20),
        name=f"ffn{layer}",
    )(xo, pa, pb, fn, an, w1, w3, w2, wq)


def solution(mesh):
    def body(x, lengths, cache, attn_norm, ffn_norm, wq, wo, w1, w3, w2):
        nb = x.shape[0]
        n_layers, _, s_len, kv = cache.shape
        nh = wq.shape[2] // kv
        ct = jnp.swapaxes(cache, 2, 3)
        order, q = _first(lengths, x, attn_norm, wq, nh)
        for l in range(n_layers):
            last = l == n_layers - 1
            pa = _attention(l, 0, q, ct, order, lengths, wo, nh)
            pa = lax.ppermute(pa, 'tp', [(0, 1), (1, 0)])
            pb = _attention(l, nb // 2, q, ct, order, lengths, wo, nh)
            res = _ffn(l, last, nh, x, pb, pa, ffn_norm, attn_norm, w1, w3, w2, wq)
            if last:
                return res[0]
            x, q = res

    in_specs = (
        P('dp', None),
        P('dp'),
        P(None, 'dp', None, None),
        P(None, None),
        P(None, None),
        P(None, None, 'tp'),
        P(None, 'tp', None),
        P(None, None, ('dp', 'tp')),
        P(None, None, ('dp', 'tp')),
        P(None, ('dp', 'tp'), None),
    )
    return jax.shard_map(body, mesh=mesh, in_specs=in_specs, out_specs=P('dp', None), check_vma=False)
```

```python
import functools

import jax
import jax.numpy as jnp
from jax import lax
from jax.experimental import pallas as pl
from jax.experimental.pallas import tpu as pltpu
from jax.sharding import PartitionSpec as P

LAT = 512
EPS = 1e-6
SCALE = 192 ** -0.5
BF = jnp.bfloat16
F32 = jnp.float32
MESH = pl.DeviceIdType.MESH
VMEM = pl.BlockSpec(memory_space=pltpu.VMEM)
SMEM = pl.BlockSpec(memory_space=pltpu.SMEM)
ANY = pl.BlockSpec(memory_space=pl.ANY)


PAD = 256


def _rmsnorm(v, w):
    vf = v.astype(F32)
    r = lax.rsqrt(jnp.mean(vf * vf, axis=-1, keepdims=True) + EPS)
    return (vf * r * w.astype(F32)).astype(BF)


def _project(h, w, j, q_ref, nb, kv):
    nblk = -(-kv // 128)
    val = jnp.dot(h, w, preferred_element_type=F32).astype(BF).astype(F32)
    lo = (kv // 128) * 128
    odd = pltpu.roll(val[:, lo:lo + nblk * 128], nblk * 128 - (kv - lo), 1)
    for t, v in ((0, val), (1, odd)):
        for i in range(nblk):
            q_ref[pl.ds(((2 * j + t) * nblk + i) * nb, nb), :] = v[:, i * 128:(i + 1) * 128]


def _first_kernel(lens_hbm, x_hbm, an_hbm, wq_ref, order_ref, q_ref, wbuf, wsem, lens_ref, x_ref, an_ref, isem):
    nb = x_ref.shape[0]
    ins = [pltpu.make_async_copy(src, dst, isem.at[i])
           for i, (src, dst) in enumerate(((lens_hbm, lens_ref), (x_hbm, x_ref), (an_hbm, an_ref)))]
    for cp in ins:
        cp.start()
    kv2 = wq_ref.shape[2] // wbuf.shape[0]
    nj = wbuf.shape[0]
    cps = [pltpu.make_async_copy(wq_ref.at[0, :, pl.ds(j * kv2, kv2)], wbuf.at[j, :, pl.ds(0, kv2)], wsem.at[j]) for j in range(nj)]
    for cp in cps:
        cp.start()
    for cp in ins:
        cp.wait()
    tp = lax.axis_index("tp").astype(F32)
    half = nb // 2
    r = lax.broadcasted_iota(jnp.int32, (nb, nb), 0).astype(F32)
    c = lax.broadcasted_iota(jnp.int32, (nb, nb), 1).astype(F32)
    rh = (r >= half).astype(F32)
    ch = (c >= half).astype(F32)
    key = jnp.broadcast_to(lens_ref[...].astype(F32), (nb, nb)) * nb + c
    mine = jnp.sum(jnp.where(r == c, key, 0.0), axis=1, keepdims=True)
    rank = jnp.sum(jnp.where((rh == ch) & (key < mine), 1.0, 0.0), axis=1, keepdims=True)
    want = jnp.where(ch == 0.0, 1.0 - tp, tp)
    hit = (rank == c - ch * half) & (rh == want)
    order_ref[0:1, :] = jnp.sum(jnp.where(hit, r, 0.0), axis=0, keepdims=True).astype(jnp.int32)
    mylen = jnp.sum(jnp.where(r == c, jnp.broadcast_to(lens_ref[...].astype(F32), (nb, nb)), 0.0), axis=1, keepdims=True)
    order_ref[1:2, :] = jnp.sum(jnp.where(hit, mylen, 0.0), axis=0, keepdims=True).astype(jnp.int32)
    h = _rmsnorm(x_ref[...], an_ref[0:1, :])
    for j in range(nj):
        cps[j].wait()
        _project(h, wbuf[j, :, 0:kv2], j, q_ref, nb, kv2 // 2)


def _first(lens, x, an, wq, nh):
    nb, d = x.shape
    kv = wq.shape[2] // nh
    return pl.pallas_call(
        _first_kernel,
        out_shape=[jax.ShapeDtypeStruct((2, nb), jnp.int32),
                   jax.ShapeDtypeStruct((-(-kv // 128) * nb * nh, 128), F32)],
        in_specs=[ANY, ANY, ANY, ANY],
        out_specs=[VMEM, VMEM],
        scratch_shapes=[pltpu.VMEM((nh // 2, d, 2 * kv + 128), BF), pltpu.SemaphoreType.DMA((nh // 2,)),
                        pltpu.VMEM((1, nb), jnp.int32), pltpu.VMEM((nb, d), BF), pltpu.VMEM(an.shape, BF),
                        pltpu.SemaphoreType.DMA((3,))],
        compiler_params=pltpu.CompilerParams(vmem_limit_bytes=32 * 2 ** 20),
        name="first",
    )(*[pltpu.with_memory_space_constraint(t, pltpu.HBM) for t in (lens.reshape(1, nb), x, an, wq)])


def _attn_kernel(layer, off, nh, G, NS, order_ref, q_ref, ct_ref, wo_ref, out_ref, *rest):
    if off == 0:
        wbuf, buf, sems, o_s, oflat, wsems = rest
    else:
        buf, sems, o_s, oflat = rest
        wbuf = wo_ref
    kv = ct_ref.shape[2]
    nmax = ct_ref.shape[3] // 128
    nb = out_ref.shape[0]
    nall = ct_ref.shape[1]
    ng = nb // G
    wrows = wbuf.shape[0] // ng
    qblk = -(-kv // 128)

    def seq(i):
        return order_ref[0, off + i]

    def length(i):
        return order_ref[1, off + i]

    def chunks(g):
        return lax.div(length(g * G + G - 1) + 127, 128)

    def copies(g, n):
        slot = lax.rem(g, NS)
        return [pltpu.make_async_copy(
            ct_ref.at[layer, seq(g * G + s), :, pl.ds(0, n * 128)],
            buf.at[slot, s, :, pl.ds(0, n * 128)],
            sems.at[slot, s]) for s in range(G)]

    def wcopy(g):
        rows = pl.ds(pl.multiple_of(g * wrows, wrows), wrows)
        return pltpu.make_async_copy(wo_ref.at[layer, rows, :], wbuf.at[rows, :], wsems.at[g])

    def start(g):
        c = chunks(g)
        for n in range(1, nmax + 1):
            @pl.when(c == n)
            def _():
                for cp in copies(g, n):
                    cp.start()

    def qrow(b):
        parts = [q_ref[pl.ds(i * nall + b, nh, stride=qblk * nall), :] for i in range(qblk)]
        return jnp.concatenate(parts, axis=-1)[:, :kv].astype(BF)

    for g in range(NS - 1):
        start(g)

    def body(g, carry):
        @pl.when(g + NS - 1 < ng)
        def _():
            start(g + NS - 1)
        if off == 0:
            wcopy(g).start()
        c = chunks(g)
        slot = lax.rem(g, NS)
        for n in range(1, nmax + 1):
            @pl.when(c == n)
            def _():
                N = n * 128
                for cp in copies(g, n):
                    cp.wait()
                bs = [seq(g * G + s) for s in range(G)]
                scs = [jnp.dot(qrow(bs[s]), buf[slot, s, :, 0:N], preferred_element_type=F32)
                       for s in range(G)]
                pos = lax.broadcasted_iota(jnp.int32, (nh, N), 1)
                scs = [jnp.where(pos < length(g * G + s), scs[s] * SCALE, -jnp.inf) for s in range(G)]
                ms = [jnp.max(sc, axis=-1, keepdims=True) for sc in scs]
                es = [jnp.exp(sc - m) for sc, m in zip(scs, ms)]
                ds = [jnp.sum(e, axis=-1, keepdims=True) for e in es]
                ps = [(e / d).astype(BF) for e, d in zip(es, ds)]
                outs = [lax.dot_general(ps[s], buf[slot, s, 0:LAT, 0:N], (((1,), (1,)), ((), ())),
                                        preferred_element_type=F32) for s in range(G)]
                for s in range(G):
                    row = lax.rem(bs[s], nb)
                    for i in range(LAT // 128):
                        o_s[pl.ds(row + i * nb, nh, stride=LAT // 128 * nb), :] = outs[s][:, i * 128:(i + 1) * 128]
        return carry

    lax.fori_loop(0, ng, body, 0)
    for h in range(nh):
        for i in range(LAT // 128):
            c = h * LAT + i * 128
            oflat[:, c:c + 128] = o_s[pl.ds((h * (LAT // 128) + i) * nb, nb), :].astype(BF)
    for g in range(ng if off == 0 else 0):
        wcopy(g).wait()
    nblk = 1024

    def mm(j, carry):
        cols = pl.ds(pl.multiple_of(j * nblk, nblk), nblk)
        out_ref[:, cols] = jnp.dot(oflat[...], wbuf[:, cols], preferred_element_type=F32)
        return carry
    lax.fori_loop(0, out_ref.shape[1] // nblk, mm, 0)


def _attention(layer, off, q, ct, order, wo, nh, G=8, NS=3):
    kv, s_len = ct.shape[2:]
    nb = order.shape[1] // 2
    hid, d = wo.shape[-2:]
    part = jax.ShapeDtypeStruct((nb, d), F32)
    return pl.pallas_call(
        functools.partial(_attn_kernel, layer, off, nh, G, NS),
        out_shape=[part, jax.ShapeDtypeStruct((hid, d), BF)] if off == 0 else part,
        in_specs=[SMEM, VMEM, ANY, ANY if off == 0 else VMEM],
        out_specs=[VMEM, VMEM] if off == 0 else VMEM,
        scratch_shapes=[
            pltpu.VMEM((NS, G, kv, s_len), BF), pltpu.SemaphoreType.DMA((NS, G)),
            pltpu.VMEM((LAT // 128 * nb * nh, 128), F32), pltpu.VMEM((nb, hid), BF),
        ] + ([pltpu.SemaphoreType.DMA((nb // G,))] if off == 0 else []),
        compiler_params=pltpu.CompilerParams(vmem_limit_bytes=24 * 2 ** 20),
        cost_estimate=pl.CostEstimate(flops=20 * 10 ** 9, bytes_accessed=40 * 2 ** 20, transcendentals=0),
        name=f"attn{layer}",
    )(order, q, ct, wo)


XLOC = {1: (1, 0), 0: (2, 0)}
YLOC = {0: (1, 1), 1: (2, 1)}
W = 512
A = (0, 1)
B = (2, 3)
QORDER = (0, 2, 1, 3)
HALF = 64


def _ffn_kernel(layer, last, nh, xo_ref, pa_ref, pb_ref, fn_ref, an_ref, w1_ref, w3_ref, w2_ref, wq_ref, *rest):
    if last:
        out_ref, rest = rest[0], rest[1:]
    else:
        xn_ref, q_ref, rest = rest[0], rest[1], rest[2:]
    (w13, w2v, wqv, gbuf, ybuf, sbuf, abuf, xp, xall,
     r1x_own, r1x_y, r1y_own, r1y_x, r2x, r2y,
     wsem, w2sem, wqsem, ss, rs) = rest
    tp = lax.axis_index("tp")
    dp = lax.axis_index("dp")
    xi, ci = lax.div(dp, 2), lax.rem(dp, 2)
    SIB = (tp, xi * 2 + 1 - ci)
    X = (tp, (1 - xi) * 2 + ci)
    Y = (1 - tp, dp)

    bar = pltpu.get_barrier_semaphore()
    for peer in (SIB, X, Y):
        pl.semaphore_signal(bar, inc=1, device_id=peer, device_id_type=MESH)

    nblk = w1_ref.shape[2] // 128
    wcopies = []
    for j in range(nblk):
        for i, w in enumerate((w3_ref, w1_ref)):
            wcopies.append(pltpu.make_async_copy(
                w.at[layer, :, pl.ds(j * 128, 128)], w13.at[:, pl.ds(j * 256 + i * 128, 128)],
                wsem.at[j, i]))
    w2copy = pltpu.make_async_copy(w2_ref.at[layer], w2v.at[:, pl.ds(0, w2_ref.shape[2])], w2sem)
    for cp in wcopies:
        cp.start()
    w2copy.start()
    nj = nh // 2
    if not last:
        kv2 = wq_ref.shape[2] // nj
        dst = [w13.at[:, pl.ds(j * kv2, kv2)] if j < 2 else wqv.at[j - 2, :, pl.ds(0, kv2)]
               for j in range(nj)]
        wqcopies = [pltpu.make_async_copy(wq_ref.at[layer + 1, :, pl.ds(j * kv2, kv2)], dst[j], wqsem.at[j])
                    for j in range(nj)]
        for cp in wqcopies[2:]:
            cp.start()

    count = [16]

    def remote(src, dst, dev, i=None):
        if i is None:
            i = count[0]
            count[0] += 1
        return pltpu.make_async_remote_copy(src_ref=src, dst_ref=dst, send_sem=ss.at[i], recv_sem=rs.at[i],
                                            device_id=dev, device_id_type=MESH)

    def cols(q):
        return pl.ds(q * W, W)

    colA, colB = pl.ds(A[0] * W, len(A) * W), pl.ds(B[0] * W, len(B) * W)
    own_sib = remote(gbuf.at[0, 0], gbuf.at[0, 1], SIB)
    own_x = {p: remote(gbuf.at[0, 0, p], gbuf.at[XLOC[p][0], 0, XLOC[p][1]], X) for p in (1, 0)}
    own_y = {p: remote(gbuf.at[0, 0, p], gbuf.at[YLOC[p][0], 0, YLOC[p][1]], Y) for p in (0, 1)}
    relay_x = remote(gbuf.at[1, 0, 1], gbuf.at[3, 0, 0], X)
    relay_y = remote(gbuf.at[1, 0, 0], gbuf.at[3, 0, 1], Y)
    sib_g = {k: remote(gbuf.at[k, 0], gbuf.at[k, 1], SIB) for k in (1, 2, 3)}
    PS = (0, 1)
    st1_x = {p: remote(ybuf.at[XLOC[p][0], 0, XLOC[p][1], :, colA], r1x_own.at[p], X) for p in PS}
    st1_y = {p: remote(ybuf.at[YLOC[p][0], 0, YLOC[p][1], :, colB], r1y_own.at[p], Y) for p in PS}
    st1_dx = {(p, q): remote(ybuf.at[3, 0, p, :, cols(q)], r1x_y.at[p, i], X) for p in PS for i, q in enumerate(A)}
    st1_dy = {(p, q): remote(ybuf.at[3, 0, p, :, cols(q)], r1y_x.at[p, i], Y) for p in PS for i, q in enumerate(B)}
    st2_y = {(p, q): remote(r1x_y.at[p, i], r2y.at[p, i], Y) for p in PS for i, q in enumerate(A)}
    st2_x = {(p, q): remote(r1y_x.at[p, i], r2x.at[p, i], X) for p in PS for i, q in enumerate(B)}
    mine = [pl.ds(pl.multiple_of(tp * HALF + p * 32, 32), 32) for p in PS]
    xg = {(p, q): remote(xall.at[mine[p], cols(q)], xall.at[mine[p], cols(q)], Y) for p in PS for q in A + B}

    def sib_y(k, q):
        return remote(ybuf.at[k, 1, :, :, cols(q)], sbuf.at[k, :, :, cols(q)], SIB, k * 4 + q)

    if xo_ref.shape[0] == HALF:
        xo = xo_ref[...]
    else:
        xo = xo_ref[pl.ds(pl.multiple_of(tp * HALF, HALF), HALF), :]
    x1 = (xo.astype(F32) + (pa_ref[...] + pb_ref[...]).astype(BF).astype(F32)).astype(BF)
    xp[...] = x1
    gbuf[0, 0] = _rmsnorm(x1, fn_ref[layer:layer + 1, :]).reshape(2, 32, -1)

    pl.semaphore_wait(bar, 3)
    own_sib.start()
    own_x[1].start()
    own_y[0].start()
    own_x[0].start()
    own_y[1].start()

    def combine(k, q):
        sib_y(k, q).wait_recv()
        ybuf[k, 0, :, :, cols(q)] = ybuf[k, 0, :, :, cols(q)] + sbuf[k, :, :, cols(q)]

    def chunk(k, carry):
        @pl.when(k == 0)
        def _():
            own_sib.wait_recv()
            for cp in wcopies:
                cp.wait()
        for kk in (1, 2, 3):
            @pl.when(k == kk)
            def _():
                sib_g[kk].wait_recv()
        g = gbuf[k].reshape(2 * HALF, -1)
        for j in range(nblk):
            uv = jnp.dot(g, w13[:, j * 256:(j + 1) * 256], preferred_element_type=F32)
            u, v = uv[:, :128], uv[:, 128:]
            abuf[:, j * 128:(j + 1) * 128] = (jax.nn.silu(u) * v).astype(BF)

        @pl.when(k == 0)
        def _():
            own_x[1].wait_recv()
            own_y[0].wait_recv()
            relay_x.start()
            relay_y.start()
            sib_g[1].start()
            w2copy.wait()

        @pl.when(k == 1)
        def _():
            own_x[0].wait_recv()
            own_y[1].wait_recv()
            sib_g[2].start()
            for q in QORDER:
                combine(0, q)

        @pl.when(k == 2)
        def _():
            relay_x.wait_recv()
            relay_y.wait_recv()
            sib_g[3].start()
            for q in QORDER:
                combine(1, q)
            st1_x[1].start()
            st1_y[0].start()

        @pl.when(k == 3)
        def _():
            if not last:
                for cp in wqcopies[:2]:
                    cp.start()
            for q in QORDER:
                combine(2, q)
            st1_x[0].start()
            st1_y[1].start()

        a = abuf[...]
        for q in QORDER:
            y = jnp.dot(a, w2v[:, q * W:(q + 1) * W], preferred_element_type=F32)
            ybuf[k, :, :, :, q * W:(q + 1) * W] = y.reshape(2, 2, 32, W)
            sib_y(k, q).start()
        return carry

    lax.fori_loop(0, 4, chunk, 0)
    for q in QORDER:
        combine(3, q)
        for p in PS:
            (st1_dx if q in A else st1_dy)[p, q].start()
    for q in QORDER:
        for p in PS:
            if q in A:
                st1_dx[p, q].wait_recv()
                (k, j), i = YLOC[p], A.index(q)
                r1x_y[p, i] = r1x_y[p, i] + ybuf[k, 0, j, :, q * W:(q + 1) * W]
                st2_y[p, q].start()
            else:
                st1_dy[p, q].wait_recv()
                (k, j), i = XLOC[p], B.index(q)
                r1y_x[p, i] = r1y_x[p, i] + ybuf[k, 0, j, :, q * W:(q + 1) * W]
                st2_x[p, q].start()
    for p in PS:
        st1_x[p].wait_recv()
        st1_y[p].wait_recv()
    for q in QORDER:
        for p in PS:
            c = slice(q * W, (q + 1) * W)
            y = ybuf[0, 0, p, :, c]
            if q in A:
                st2_y[p, q].wait_recv()
                i = A.index(q)
                y = y + r1x_own[p, :, i * W:(i + 1) * W] + r2y[p, i]
            else:
                st2_x[p, q].wait_recv()
                i = B.index(q)
                y = y + r1y_own[p, :, i * W:(i + 1) * W] + r2x[p, i]
            xn = (xp[p * 32:(p + 1) * 32, c].astype(F32) + y.astype(BF).astype(F32)).astype(BF)
            xall[mine[p], c] = xn
            if not last:
                xn_ref[p * 32:(p + 1) * 32, c] = xn
            xg[p, q].start()
    for cp in xg.values():
        cp.wait_recv()
    if last:
        out_ref[...] = xall[...]
    else:
        h = _rmsnorm(xall[...], an_ref[layer + 1:layer + 2, :])
        for j, cp in enumerate(wqcopies):
            cp.wait()
            _project(h, dst[j][...], j, q_ref, 2 * HALF, kv2 // 2)
    for cp in [own_sib, relay_x, relay_y, *own_x.values(), *own_y.values(), *sib_g.values(),
               *st1_x.values(), *st1_y.values(), *st1_dx.values(), *st1_dy.values(),
               *st2_x.values(), *st2_y.values(), *xg.values()]:
        cp.wait_send()
    for k in range(4):
        for q in QORDER:
            sib_y(k, q).wait_send()


NCOPY = 16 + 10 + 4 + 8 + 8 + 8


def _ffn(layer, last, nh, xo, pa, pb, fn, an, w1, w3, w2, wq):
    rows, d = pa.shape
    f = w1.shape[2]
    kv = wq.shape[2] // nh
    if last:
        out_shape = [jax.ShapeDtypeStruct((2 * rows, d), BF)]
    else:
        out_shape = [jax.ShapeDtypeStruct((rows, d), BF),
                     jax.ShapeDtypeStruct((-(-kv // 128) * 2 * rows * nh, 128), F32)]
    NA, NB = len(A), len(B)
    scratch = [
        pltpu.VMEM((d, 2 * f), BF), pltpu.VMEM((f, d + PAD), BF),
        pltpu.VMEM((1, 16, 128) if last else (nh // 2 - 2, d, 2 * kv + 128), BF),
        pltpu.VMEM((4, 2, 2, 32, d), BF), pltpu.VMEM((4, 2, 2, 32, d), F32), pltpu.VMEM((4, 2, 32, d), F32),
        pltpu.VMEM((128, f), BF), pltpu.VMEM((rows, d), BF), pltpu.VMEM((2 * rows, d), BF),
        pltpu.VMEM((2, 32, NA * W), F32), pltpu.VMEM((2, NA, 32, W), F32),
        pltpu.VMEM((2, 32, NB * W), F32), pltpu.VMEM((2, NB, 32, W), F32),
        pltpu.VMEM((2, NB, 32, W), F32), pltpu.VMEM((2, NA, 32, W), F32),
        pltpu.SemaphoreType.DMA((f // 128, 2)), pltpu.SemaphoreType.DMA, pltpu.SemaphoreType.DMA((nh // 2,)),
        pltpu.SemaphoreType.DMA((NCOPY,)), pltpu.SemaphoreType.DMA((NCOPY,)),
    ]
    return pl.pallas_call(
        functools.partial(_ffn_kernel, layer, last, nh),
        out_shape=out_shape,
        in_specs=[VMEM, VMEM, VMEM, VMEM, VMEM, ANY, ANY, ANY, ANY],
        out_specs=[VMEM] * len(out_shape),
        scratch_shapes=scratch,
        compiler_params=pltpu.CompilerParams(collective_id=layer, has_side_effects=True,
                                             vmem_limit_bytes=48 * 2 ** 20),
        name=f"ffn{layer}",
    )(xo, pa, pb, fn, an, w1, w3, w2, wq)


def solution(mesh):
    def body(x, lengths, cache, attn_norm, ffn_norm, wq, wo, w1, w3, w2):
        nb = x.shape[0]
        n_layers, _, s_len, kv = cache.shape
        nh = wq.shape[2] // kv
        ct = jnp.swapaxes(cache, 2, 3)
        order, q = _first(lengths, x, attn_norm, wq, nh)
        for l in range(n_layers):
            last = l == n_layers - 1
            pa, wo_l = _attention(l, 0, q, ct, order, wo, nh)
            pa = lax.ppermute(pa, 'tp', [(0, 1), (1, 0)])
            pb = _attention(l, nb // 2, q, ct, order, wo_l, nh)
            res = _ffn(l, last, nh, x, pb, pa, ffn_norm, attn_norm, w1, w3, w2, wq)
            if last:
                return res[0]
            x, q = res

    in_specs = (
        P('dp', None),
        P('dp'),
        P(None, 'dp', None, None),
        P(None, None),
        P(None, None),
        P(None, None, 'tp'),
        P(None, 'tp', None),
        P(None, None, ('dp', 'tp')),
        P(None, None, ('dp', 'tp')),
        P(None, ('dp', 'tp'), None),
    )
    return jax.shard_map(body, mesh=mesh, in_specs=in_specs, out_specs=P('dp', None), check_vma=False)
```

```python
import functools

import jax
import jax.numpy as jnp
from jax import lax
from jax.experimental import pallas as pl
from jax.experimental.pallas import tpu as pltpu
from jax.sharding import PartitionSpec as P

LAT = 512
EPS = 1e-6
SCALE = 192 ** -0.5
BF = jnp.bfloat16
F32 = jnp.float32
MESH = pl.DeviceIdType.MESH
VMEM = pl.BlockSpec(memory_space=pltpu.VMEM)
SMEM = pl.BlockSpec(memory_space=pltpu.SMEM)
ANY = pl.BlockSpec(memory_space=pl.ANY)


def _rmsnorm(v, w):
    vf = v.astype(F32)
    r = lax.rsqrt(jnp.mean(vf * vf, axis=-1, keepdims=True) + EPS)
    return (vf * r * w.astype(F32)).astype(BF)


def _project(h, w, j, q_ref, nb, kv):
    nblk = -(-kv // 128)
    val = jnp.dot(h, w, preferred_element_type=F32).astype(BF).astype(F32)
    lo = (kv // 128) * 128
    odd = pltpu.roll(val[:, lo:lo + nblk * 128], nblk * 128 - (kv - lo), 1)
    for t, v in ((0, val), (1, odd)):
        for i in range(nblk):
            q_ref[pl.ds(((2 * j + t) * nblk + i) * nb, nb), :] = v[:, i * 128:(i + 1) * 128]


def _first_kernel(lens_hbm, x_hbm, an_hbm, wq_ref, order_ref, q_ref, wbuf, wsem, lens_ref, x_ref, an_ref, isem):
    nb = x_ref.shape[0]
    ins = [pltpu.make_async_copy(src, dst, isem.at[i])
           for i, (src, dst) in enumerate(((lens_hbm, lens_ref), (x_hbm, x_ref), (an_hbm, an_ref)))]
    for cp in ins:
        cp.start()
    kv2 = wq_ref.shape[2] // wbuf.shape[0]
    nj = wbuf.shape[0]
    cps = [pltpu.make_async_copy(wq_ref.at[0, :, pl.ds(j * kv2, kv2)], wbuf.at[j, :, pl.ds(0, kv2)], wsem.at[j]) for j in range(nj)]
    for cp in cps:
        cp.start()
    for cp in ins:
        cp.wait()
    tp = lax.axis_index("tp").astype(F32)
    half = nb // 2
    r = lax.broadcasted_iota(jnp.int32, (nb, nb), 0).astype(F32)
    c = lax.broadcasted_iota(jnp.int32, (nb, nb), 1).astype(F32)
    rh = (r >= half).astype(F32)
    ch = (c >= half).astype(F32)
    key = jnp.broadcast_to(lens_ref[...].astype(F32), (nb, nb)) * nb + c
    mine = jnp.sum(jnp.where(r == c, key, 0.0), axis=1, keepdims=True)
    rank = jnp.sum(jnp.where((rh == ch) & (key < mine), 1.0, 0.0), axis=1, keepdims=True)
    want = jnp.where(ch == 0.0, 1.0 - tp, tp)
    hit = (rank == c - ch * half) & (rh == want)
    order_ref[0:1, :] = jnp.sum(jnp.where(hit, r, 0.0), axis=0, keepdims=True).astype(jnp.int32)
    mylen = jnp.sum(jnp.where(r == c, jnp.broadcast_to(lens_ref[...].astype(F32), (nb, nb)), 0.0), axis=1, keepdims=True)
    order_ref[1:2, :] = jnp.sum(jnp.where(hit, mylen, 0.0), axis=0, keepdims=True).astype(jnp.int32)
    h = _rmsnorm(x_ref[...], an_ref[0:1, :])
    for j in range(nj):
        cps[j].wait()
        _project(h, wbuf[j, :, 0:kv2], j, q_ref, nb, kv2 // 2)


def _first(lens, x, an, wq, nh):
    nb, d = x.shape
    kv = wq.shape[2] // nh
    return pl.pallas_call(
        _first_kernel,
        out_shape=[jax.ShapeDtypeStruct((2, nb), jnp.int32),
                   jax.ShapeDtypeStruct((-(-kv // 128) * nb * nh, 128), F32)],
        in_specs=[ANY, ANY, ANY, ANY],
        out_specs=[VMEM, VMEM],
        scratch_shapes=[pltpu.VMEM((nh // 2, d, 2 * kv + 128), BF), pltpu.SemaphoreType.DMA((nh // 2,)),
                        pltpu.VMEM((1, nb), jnp.int32), pltpu.VMEM((nb, d), BF), pltpu.VMEM(an.shape, BF),
                        pltpu.SemaphoreType.DMA((3,))],
        compiler_params=pltpu.CompilerParams(vmem_limit_bytes=32 * 2 ** 20),
        name="first",
    )(*[pltpu.with_memory_space_constraint(t, pltpu.HBM) for t in (lens.reshape(1, nb), x, an)], wq)


def _attn_kernel(layer, off, load, nh, G, NS, order_ref, q_ref, ct_ref, wo_ref, *rest):
    if load:
        out_ref, buf, wbuf, sems, o_s, oflat, wsems = rest
    else:
        out_ref, buf, sems, o_s, oflat = rest if off == 0 else rest[1:]
        wbuf = wo_ref
    kv = ct_ref.shape[2]
    nmax = ct_ref.shape[3] // 128
    nb = out_ref.shape[0]
    nall = ct_ref.shape[1]
    ng = nb // G
    wrows = wbuf.shape[0] // ng
    qblk = -(-kv // 128)

    base = off // G
    ahead = NS - 1

    def seq(i):
        return order_ref[0, i]

    def length(i):
        return order_ref[1, i]

    def chunks(g):
        return lax.div(length(g * G + G - 1) + 127, 128)

    def copies(g, n):
        slot = lax.rem(g, NS)
        return [pltpu.make_async_copy(
            ct_ref.at[layer, seq(g * G + s), :, pl.ds(0, n * 128)],
            buf.at[slot, s, :, pl.ds(0, n * 128)],
            sems.at[slot, s]) for s in range(G)]

    def wcopy(g):
        rows = pl.ds(pl.multiple_of(g * wrows, wrows), wrows)
        return pltpu.make_async_copy(wo_ref.at[layer, rows, :], wbuf.at[rows, :], wsems.at[g])

    def start(g):
        c = chunks(g)
        for n in range(1, nmax + 1):
            @pl.when(c == n)
            def _():
                for cp in copies(g, n):
                    cp.start()

    def qrow(b):
        parts = [q_ref[pl.ds(i * nall + b, nh, stride=qblk * nall), :] for i in range(qblk)]
        return jnp.concatenate(parts, axis=-1)[:, :kv].astype(BF)

    if off == 0:
        for g in range(ahead):
            start(g)

    def body(g, carry):
        if off == 0:
            start(g + ahead)
            if load:
                wcopy(g).start()
        else:
            @pl.when(g + ahead < base + ng)
            def _():
                start(g + ahead)
        c = chunks(g)
        slot = lax.rem(g, NS)
        for n in range(1, nmax + 1):
            @pl.when(c == n)
            def _():
                N = n * 128
                def arrived():
                    for cp in copies(g, n):
                        cp.wait()
                if off == 0:
                    arrived()
                else:
                    pl.when(g >= base + ahead)(arrived)
                bs = [seq(g * G + s) for s in range(G)]
                scs = [jnp.dot(qrow(bs[s]), buf[slot, s, :, 0:N], preferred_element_type=F32)
                       for s in range(G)]
                pos = lax.broadcasted_iota(jnp.int32, (nh, N), 1)
                scs = [jnp.where(pos < length(g * G + s), scs[s] * SCALE, -jnp.inf) for s in range(G)]
                ms = [jnp.max(sc, axis=-1, keepdims=True) for sc in scs]
                es = [jnp.exp(sc - m) for sc, m in zip(scs, ms)]
                ds = [jnp.sum(e, axis=-1, keepdims=True) for e in es]
                ps = [(e / d).astype(BF) for e, d in zip(es, ds)]
                outs = [lax.dot_general(ps[s], buf[slot, s, 0:LAT, 0:N], (((1,), (1,)), ((), ())),
                                        preferred_element_type=F32) for s in range(G)]
                for s in range(G):
                    row = lax.rem(bs[s], nb)
                    for i in range(LAT // 128):
                        o_s[pl.ds(row + i * nb, nh, stride=LAT // 128 * nb), :] = outs[s][:, i * 128:(i + 1) * 128]
        return carry

    lax.fori_loop(base, base + ng, body, 0)
    for h in range(nh):
        for i in range(LAT // 128):
            c = h * LAT + i * 128
            oflat[:, c:c + 128] = o_s[pl.ds((h * (LAT // 128) + i) * nb, nb), :].astype(BF)
    if off == 0:
        for g in range(ng if load else 0):
            wcopy(g).wait()
        for g in range(ng, ng + ahead):
            c = chunks(g)
            for n in range(1, nmax + 1):
                @pl.when(c == n)
                def _():
                    for cp in copies(g, n):
                        cp.wait()
    nblk = 1024

    def mm(j, carry):
        cols = pl.ds(pl.multiple_of(j * nblk, nblk), nblk)
        out_ref[:, cols] = jnp.dot(oflat[...], wbuf[:, cols], preferred_element_type=F32)
        return carry
    lax.fori_loop(0, out_ref.shape[1] // nblk, mm, 0)


def _attention(layer, off, q, ct, order, wo, nh, ring=None, G=8, NS=3):
    kv, s_len = ct.shape[2:]
    nb = order.shape[1] // 2
    hid, d = wo.shape[-2:]
    first = off == 0
    load = wo.ndim == 3
    part = jax.ShapeDtypeStruct((nb, d), F32)
    rings = jax.ShapeDtypeStruct((NS, G, kv, s_len), BF)
    return pl.pallas_call(
        functools.partial(_attn_kernel, layer, off, load, nh, G, NS),
        out_shape=[part, rings] + ([jax.ShapeDtypeStruct((hid, d), BF)] if load else []),
        in_specs=[SMEM, VMEM, ANY, ANY if load else VMEM] + ([] if first else [VMEM]),
        out_specs=[VMEM] * (3 if load else 2),
        input_output_aliases={} if first else {4: 1},
        scratch_shapes=[
            pltpu.SemaphoreType.DMA((NS, G)),
            pltpu.VMEM((LAT // 128 * nb * nh, 128), F32), pltpu.VMEM((nb, hid), BF),
        ] + ([pltpu.SemaphoreType.DMA((nb // G,))] if load else []),
        compiler_params=pltpu.CompilerParams(vmem_limit_bytes=8 * 2 ** 20),
        cost_estimate=pl.CostEstimate(flops=20 * 10 ** 9, bytes_accessed=40 * 2 ** 20, transcendentals=0),
        name=f"attn{layer}",
    )(order, q, ct, wo, *([] if first else [ring]))


XLOC = {1: (1, 0), 0: (2, 0)}
YLOC = {0: (1, 1), 1: (2, 1)}
W = 512
A = (0, 1)
B = (2, 3)
QORDER = (0, 2, 1, 3)
HALF = 64


def _ffn_kernel(layer, last, nh, xo_ref, pa_ref, pb_ref, fn_ref, an_ref, w1_ref, w3_ref, w2_ref, wq_ref, wo_ref, *rest):
    if last:
        out_ref, rest = rest[0], rest[1:]
    else:
        xn_ref, q_ref, won_ref, rest = rest[0], rest[1], rest[2], rest[3:]
    (w13, w2b, gbuf, ybuf, sbuf, abuf, xp, xall,
     r1x_own, r1x_y, r1y_own, r1y_x, r2x, r2y,
     wsem, w2sem, wqsem, wosem, ss, rs) = rest
    tp = lax.axis_index("tp")
    dp = lax.axis_index("dp")
    xi, ci = lax.div(dp, 2), lax.rem(dp, 2)
    SIB = (tp, xi * 2 + 1 - ci)
    X = (tp, (1 - xi) * 2 + ci)
    Y = (1 - tp, dp)

    bar = pltpu.get_barrier_semaphore()
    for peer in (SIB, X, Y):
        pl.semaphore_signal(bar, inc=1, device_id=peer, device_id_type=MESH)

    nblk = w1_ref.shape[2] // 128
    wcopies = []
    for j in range(nblk):
        for i, w in enumerate((w3_ref, w1_ref)):
            wcopies.append(pltpu.make_async_copy(
                w.at[layer, :, pl.ds(j * 128, 128)], w13.at[:, pl.ds(j * 256 + i * 128, 128)],
                wsem.at[j, i]))
    w2copy = pltpu.make_async_copy(w2_ref.at[layer], w2b.at[pl.ds(0, w2_ref.shape[1]), pl.ds(0, w2_ref.shape[2])], w2sem)
    for cp in wcopies:
        cp.start()
    w2copy.start()
    nj = nh // 2
    if not last:
        kv2 = wq_ref.shape[2] // nj
        dst = [(w13 if j < 2 else w2b).at[:, pl.ds(j % 2 * kv2, kv2)] for j in range(nj)]
        wqcopies = [pltpu.make_async_copy(wq_ref.at[layer + 1, :, pl.ds(j * kv2, kv2)], dst[j], wqsem.at[j])
                    for j in range(nj)]
        wocopy = pltpu.make_async_copy(wo_ref.at[layer + 1], won_ref, wosem)

    count = [16]

    def remote(src, dst, dev, i=None):
        if i is None:
            i = count[0]
            count[0] += 1
        return pltpu.make_async_remote_copy(src_ref=src, dst_ref=dst, send_sem=ss.at[i], recv_sem=rs.at[i],
                                            device_id=dev, device_id_type=MESH)

    def cols(q):
        return pl.ds(q * W, W)

    colA, colB = pl.ds(A[0] * W, len(A) * W), pl.ds(B[0] * W, len(B) * W)
    own_sib = remote(gbuf.at[0, 0], gbuf.at[0, 1], SIB)
    own_x = {p: remote(gbuf.at[0, 0, p], gbuf.at[XLOC[p][0], 0, XLOC[p][1]], X) for p in (1, 0)}
    own_y = {p: remote(gbuf.at[0, 0, p], gbuf.at[YLOC[p][0], 0, YLOC[p][1]], Y) for p in (0, 1)}
    relay_x = remote(gbuf.at[1, 0, 1], gbuf.at[3, 0, 0], X)
    relay_y = remote(gbuf.at[1, 0, 0], gbuf.at[3, 0, 1], Y)
    sib_g = {k: remote(gbuf.at[k, 0], gbuf.at[k, 1], SIB) for k in (1, 2, 3)}
    PS = (0, 1)
    st1_x = {p: remote(ybuf.at[XLOC[p][0], 0, XLOC[p][1], :, colA], r1x_own.at[p], X) for p in PS}
    st1_y = {p: remote(ybuf.at[YLOC[p][0], 0, YLOC[p][1], :, colB], r1y_own.at[p], Y) for p in PS}
    st1_dx = {(p, q): remote(ybuf.at[3, 0, p, :, cols(q)], r1x_y.at[p, i], X) for p in PS for i, q in enumerate(A)}
    st1_dy = {(p, q): remote(ybuf.at[3, 0, p, :, cols(q)], r1y_x.at[p, i], Y) for p in PS for i, q in enumerate(B)}
    st2_y = {(p, q): remote(r1x_y.at[p, i], r2y.at[p, i], Y) for p in PS for i, q in enumerate(A)}
    st2_x = {(p, q): remote(r1y_x.at[p, i], r2x.at[p, i], X) for p in PS for i, q in enumerate(B)}
    mine = [pl.ds(pl.multiple_of(tp * HALF + p * 32, 32), 32) for p in PS]
    xg = {(p, q): remote(xall.at[mine[p], cols(q)], xall.at[mine[p], cols(q)], Y) for p in PS for q in A + B}

    def sib_y(k, q):
        return remote(ybuf.at[k, 1, :, :, cols(q)], sbuf.at[k, :, :, cols(q)], SIB, k * 4 + q)

    if xo_ref.shape[0] == HALF:
        xo = xo_ref[...]
    else:
        xo = xo_ref[pl.ds(pl.multiple_of(tp * HALF, HALF), HALF), :]
    x1 = (xo.astype(F32) + (pa_ref[...] + pb_ref[...]).astype(BF).astype(F32)).astype(BF)
    xp[...] = x1
    gbuf[0, 0] = _rmsnorm(x1, fn_ref[layer:layer + 1, :]).reshape(2, 32, -1)

    pl.semaphore_wait(bar, 3)
    own_sib.start()
    own_x[1].start()
    own_y[0].start()
    own_x[0].start()
    own_y[1].start()

    def combine(k, q):
        sib_y(k, q).wait_recv()
        ybuf[k, 0, :, :, cols(q)] = ybuf[k, 0, :, :, cols(q)] + sbuf[k, :, :, cols(q)]

    def chunk(k, carry):
        @pl.when(k == 0)
        def _():
            own_sib.wait_recv()
            for cp in wcopies:
                cp.wait()
        for kk in (1, 2, 3):
            @pl.when(k == kk)
            def _():
                sib_g[kk].wait_recv()
        g = gbuf[k].reshape(2 * HALF, -1)
        for j in range(nblk):
            uv = jnp.dot(g, w13[:, j * 256:(j + 1) * 256], preferred_element_type=F32)
            u, v = uv[:, :128], uv[:, 128:]
            abuf[:, j * 128:(j + 1) * 128] = (jax.nn.silu(u) * v).astype(BF)

        @pl.when(k == 0)
        def _():
            own_x[1].wait_recv()
            own_y[0].wait_recv()
            relay_x.start()
            relay_y.start()
            sib_g[1].start()
            w2copy.wait()

        @pl.when(k == 1)
        def _():
            own_x[0].wait_recv()
            own_y[1].wait_recv()
            sib_g[2].start()
            for q in QORDER:
                combine(0, q)

        @pl.when(k == 2)
        def _():
            relay_x.wait_recv()
            relay_y.wait_recv()
            sib_g[3].start()
            for q in QORDER:
                combine(1, q)
            st1_x[1].start()
            st1_y[0].start()

        @pl.when(k == 3)
        def _():
            if not last:
                for cp in wqcopies[:2]:
                    cp.start()
            for q in QORDER:
                combine(2, q)
            st1_x[0].start()
            st1_y[1].start()

        a = abuf[...]
        for q in QORDER:
            y = jnp.dot(a, w2b[0:w2_ref.shape[1], q * W:(q + 1) * W], preferred_element_type=F32)
            ybuf[k, :, :, :, q * W:(q + 1) * W] = y.reshape(2, 2, 32, W)
            sib_y(k, q).start()
        return carry

    lax.fori_loop(0, 4, chunk, 0)
    if not last:
        for cp in wqcopies[2:]:
            cp.start()
        wocopy.start()
    for q in QORDER:
        combine(3, q)
        for p in PS:
            (st1_dx if q in A else st1_dy)[p, q].start()
    for q in QORDER:
        for p in PS:
            if q in A:
                st1_dx[p, q].wait_recv()
                (k, j), i = YLOC[p], A.index(q)
                r1x_y[p, i] = r1x_y[p, i] + ybuf[k, 0, j, :, q * W:(q + 1) * W]
                st2_y[p, q].start()
            else:
                st1_dy[p, q].wait_recv()
                (k, j), i = XLOC[p], B.index(q)
                r1y_x[p, i] = r1y_x[p, i] + ybuf[k, 0, j, :, q * W:(q + 1) * W]
                st2_x[p, q].start()
    for p in PS:
        st1_x[p].wait_recv()
        st1_y[p].wait_recv()
    for q in QORDER:
        for p in PS:
            c = slice(q * W, (q + 1) * W)
            y = ybuf[0, 0, p, :, c]
            if q in A:
                st2_y[p, q].wait_recv()
                i = A.index(q)
                y = y + r1x_own[p, :, i * W:(i + 1) * W] + r2y[p, i]
            else:
                st2_x[p, q].wait_recv()
                i = B.index(q)
                y = y + r1y_own[p, :, i * W:(i + 1) * W] + r2x[p, i]
            xn = (xp[p * 32:(p + 1) * 32, c].astype(F32) + y.astype(BF).astype(F32)).astype(BF)
            xall[mine[p], c] = xn
            if not last:
                xn_ref[p * 32:(p + 1) * 32, c] = xn
            xg[p, q].start()
    for cp in xg.values():
        cp.wait_recv()
    if last:
        out_ref[...] = xall[...]
    else:
        h = _rmsnorm(xall[...], an_ref[layer + 1:layer + 2, :])
        for j, cp in enumerate(wqcopies):
            cp.wait()
            _project(h, dst[j][...], j, q_ref, 2 * HALF, kv2 // 2)
    if not last:
        wocopy.wait()
    for cp in [own_sib, relay_x, relay_y, *own_x.values(), *own_y.values(), *sib_g.values(),
               *st1_x.values(), *st1_y.values(), *st1_dx.values(), *st1_dy.values(),
               *st2_x.values(), *st2_y.values(), *xg.values()]:
        cp.wait_send()
    for k in range(4):
        for q in QORDER:
            sib_y(k, q).wait_send()


NCOPY = 16 + 10 + 4 + 8 + 8 + 8


def _ffn(layer, last, nh, xo, pa, pb, fn, an, w1, w3, w2, wq, wo):
    rows, d = pa.shape
    f = w1.shape[2]
    kv = wq.shape[2] // nh
    if last:
        out_shape = [jax.ShapeDtypeStruct((2 * rows, d), BF)]
    else:
        out_shape = [jax.ShapeDtypeStruct((rows, d), BF),
                     jax.ShapeDtypeStruct((-(-kv // 128) * 2 * rows * nh, 128), F32),
                     jax.ShapeDtypeStruct(wo.shape[1:], BF)]
    NA, NB = len(A), len(B)
    scratch = [
        pltpu.VMEM((d, 2 * f), BF), pltpu.VMEM((f, d) if last else (d, 4 * kv), BF),
        pltpu.VMEM((4, 2, 2, 32, d), BF), pltpu.VMEM((4, 2, 2, 32, d), F32), pltpu.VMEM((4, 2, 32, d), F32),
        pltpu.VMEM((128, f), BF), pltpu.VMEM((rows, d), BF), pltpu.VMEM((2 * rows, d), BF),
        pltpu.VMEM((2, 32, NA * W), F32), pltpu.VMEM((2, NA, 32, W), F32),
        pltpu.VMEM((2, 32, NB * W), F32), pltpu.VMEM((2, NB, 32, W), F32),
        pltpu.VMEM((2, NB, 32, W), F32), pltpu.VMEM((2, NA, 32, W), F32),
        pltpu.SemaphoreType.DMA((f // 128, 2)), pltpu.SemaphoreType.DMA, pltpu.SemaphoreType.DMA((nh // 2,)),
        pltpu.SemaphoreType.DMA, pltpu.SemaphoreType.DMA((NCOPY,)), pltpu.SemaphoreType.DMA((NCOPY,)),
    ]
    return pl.pallas_call(
        functools.partial(_ffn_kernel, layer, last, nh),
        out_shape=out_shape,
        in_specs=[VMEM, VMEM, VMEM, VMEM, VMEM, ANY, ANY, ANY, ANY, ANY],
        out_specs=[VMEM] * len(out_shape),
        scratch_shapes=scratch,
        compiler_params=pltpu.CompilerParams(collective_id=layer, has_side_effects=True,
                                             vmem_limit_bytes=65 * 2 ** 19),
        name=f"ffn{layer}",
    )(xo, pa, pb, fn, an, w1, w3, w2, wq, wo)


def solution(mesh):
    def body(x, lengths, cache, attn_norm, ffn_norm, wq, wo, w1, w3, w2):
        nb = x.shape[0]
        n_layers, _, s_len, kv = cache.shape
        nh = wq.shape[2] // kv
        ct = jnp.swapaxes(cache, 2, 3)
        ct, wq, wo, w1, w3, w2 = [pltpu.with_memory_space_constraint(t, pltpu.HBM) for t in (ct, wq, wo, w1, w3, w2)]
        order, q = _first(lengths, x, attn_norm, wq, nh)
        for l in range(n_layers):
            last = l == n_layers - 1
            if l == 0:
                pa, ring, wo_l = _attention(l, 0, q, ct, order, wo, nh)
            else:
                pa, ring = _attention(l, 0, q, ct, order, wo_l, nh)
            pa = lax.ppermute(pa, 'tp', [(0, 1), (1, 0)])
            pb, _ = _attention(l, nb // 2, q, ct, order, wo_l, nh, ring)
            res = _ffn(l, last, nh, x, pb, pa, ffn_norm, attn_norm, w1, w3, w2, wq, wo)
            if last:
                return res[0]
            x, q, wo_l = res

    in_specs = (
        P('dp', None),
        P('dp'),
        P(None, 'dp', None, None),
        P(None, None),
        P(None, None),
        P(None, None, 'tp'),
        P(None, 'tp', None),
        P(None, None, ('dp', 'tp')),
        P(None, None, ('dp', 'tp')),
        P(None, ('dp', 'tp'), None),
    )
    return jax.shard_map(body, mesh=mesh, in_specs=in_specs, out_specs=P('dp', None), check_vma=False)
```

```python
import functools

import jax
import jax.numpy as jnp
from jax import lax
from jax.experimental import pallas as pl
from jax.experimental.pallas import tpu as pltpu
from jax.sharding import PartitionSpec as P

LAT = 512
EPS = 1e-6
SCALE = 192 ** -0.5
BF = jnp.bfloat16
F32 = jnp.float32
MESH = pl.DeviceIdType.MESH
VMEM = pl.BlockSpec(memory_space=pltpu.VMEM)
SMEM = pl.BlockSpec(memory_space=pltpu.SMEM)
ANY = pl.BlockSpec(memory_space=pl.ANY)


def _rmsnorm(v, w):
    vf = v.astype(F32)
    r = lax.rsqrt(jnp.mean(vf * vf, axis=-1, keepdims=True) + EPS)
    return (vf * r * w.astype(F32)).astype(BF)


def _project(h, w, j, q_ref, nb, kv):
    nblk = -(-kv // 128)
    val = jnp.dot(h, w, preferred_element_type=F32).astype(BF).astype(F32)
    lo = (kv // 128) * 128
    odd = pltpu.roll(val[:, lo:lo + nblk * 128], nblk * 128 - (kv - lo), 1)
    for t, v in ((0, val), (1, odd)):
        for i in range(nblk):
            q_ref[pl.ds(((2 * j + t) * nblk + i) * nb, nb), :] = v[:, i * 128:(i + 1) * 128]


def _first_kernel(lens_hbm, x_hbm, an_hbm, wq_ref, order_ref, q_ref, wbuf, wsem, lens_ref, x_ref, an_ref, isem):
    nb = x_ref.shape[0]
    ins = [pltpu.make_async_copy(src, dst, isem.at[i])
           for i, (src, dst) in enumerate(((lens_hbm, lens_ref), (x_hbm, x_ref), (an_hbm, an_ref)))]
    for cp in ins:
        cp.start()
    kv2 = wq_ref.shape[2] // wbuf.shape[0]
    nj = wbuf.shape[0]
    cps = [pltpu.make_async_copy(wq_ref.at[0, :, pl.ds(j * kv2, kv2)], wbuf.at[j, :, pl.ds(0, kv2)], wsem.at[j]) for j in range(nj)]
    for cp in cps:
        cp.start()
    for cp in ins:
        cp.wait()
    tp = lax.axis_index("tp").astype(F32)
    half = nb // 2
    r = lax.broadcasted_iota(jnp.int32, (nb, nb), 0).astype(F32)
    c = lax.broadcasted_iota(jnp.int32, (nb, nb), 1).astype(F32)
    rh = (r >= half).astype(F32)
    ch = (c >= half).astype(F32)
    key = jnp.broadcast_to(lens_ref[...].astype(F32), (nb, nb)) * nb + c
    mine = jnp.sum(jnp.where(r == c, key, 0.0), axis=1, keepdims=True)
    rank = jnp.sum(jnp.where((rh == ch) & (key < mine), 1.0, 0.0), axis=1, keepdims=True)
    want = jnp.where(ch == 0.0, 1.0 - tp, tp)
    hit = (rank == c - ch * half) & (rh == want)
    order_ref[0:1, :] = jnp.sum(jnp.where(hit, r, 0.0), axis=0, keepdims=True).astype(jnp.int32)
    mylen = jnp.sum(jnp.where(r == c, jnp.broadcast_to(lens_ref[...].astype(F32), (nb, nb)), 0.0), axis=1, keepdims=True)
    order_ref[1:2, :] = jnp.sum(jnp.where(hit, mylen, 0.0), axis=0, keepdims=True).astype(jnp.int32)
    h = _rmsnorm(x_ref[...], an_ref[0:1, :])
    for j in range(nj):
        cps[j].wait()
        _project(h, wbuf[j, :, 0:kv2], j, q_ref, nb, kv2 // 2)


def _first(lens, x, an, wq, nh):
    nb, d = x.shape
    kv = wq.shape[2] // nh
    return pl.pallas_call(
        _first_kernel,
        out_shape=[jax.ShapeDtypeStruct((2, nb), jnp.int32),
                   jax.ShapeDtypeStruct((-(-kv // 128) * nb * nh, 128), F32)],
        in_specs=[ANY, ANY, ANY, ANY],
        out_specs=[VMEM, VMEM],
        scratch_shapes=[pltpu.VMEM((nh // 2, d, 2 * kv + 128), BF), pltpu.SemaphoreType.DMA((nh // 2,)),
                        pltpu.VMEM((1, nb), jnp.int32), pltpu.VMEM((nb, d), BF), pltpu.VMEM(an.shape, BF),
                        pltpu.SemaphoreType.DMA((3,))],
        compiler_params=pltpu.CompilerParams(vmem_limit_bytes=32 * 2 ** 20),
        name="first",
    )(*[pltpu.with_memory_space_constraint(t, pltpu.HBM) for t in (lens.reshape(1, nb), x, an)], wq)


def _attn_kernel(layer, off, load, nh, G, NS, order_ref, q_ref, ct_ref, wo_ref, out_ref, *rest):
    if load:
        wbuf, buf, sems, o_s, oflat, wsems = rest
    else:
        buf, sems, o_s, oflat = rest
        wbuf = wo_ref
    kv = ct_ref.shape[2]
    nmax = ct_ref.shape[3] // 128
    nb = out_ref.shape[0]
    nall = ct_ref.shape[1]
    ng = nb // G
    wrows = wbuf.shape[0] // ng
    qblk = -(-kv // 128)

    def seq(i):
        return order_ref[0, off + i]

    def length(i):
        return order_ref[1, off + i]

    def chunks(g):
        return lax.div(length(g * G + G - 1) + 127, 128)

    def copies(g, n):
        slot = lax.rem(g, NS)
        return [pltpu.make_async_copy(
            ct_ref.at[layer, seq(g * G + s), :, pl.ds(0, n * 128)],
            buf.at[slot, s, :, pl.ds(0, n * 128)],
            sems.at[slot, s]) for s in range(G)]

    def wcopy(g):
        rows = pl.ds(pl.multiple_of(g * wrows, wrows), wrows)
        return pltpu.make_async_copy(wo_ref.at[layer, rows, :], wbuf.at[rows, :], wsems.at[g])

    def start(g):
        c = chunks(g)
        for n in range(1, nmax + 1):
            @pl.when(c == n)
            def _():
                for cp in copies(g, n):
                    cp.start()

    def qrow(b):
        parts = [q_ref[pl.ds(i * nall + b, nh, stride=qblk * nall), :] for i in range(qblk)]
        return jnp.concatenate(parts, axis=-1)[:, :kv].astype(BF)

    for g in range(NS - 1):
        start(g)

    def body(g, carry):
        @pl.when(g + NS - 1 < ng)
        def _():
            start(g + NS - 1)
        if load:
            wcopy(g).start()
        c = chunks(g)
        slot = lax.rem(g, NS)
        for n in range(1, nmax + 1):
            @pl.when(c == n)
            def _():
                N = n * 128
                for cp in copies(g, n):
                    cp.wait()
                bs = [seq(g * G + s) for s in range(G)]
                scs = [jnp.dot(qrow(bs[s]), buf[slot, s, :, 0:N], preferred_element_type=F32)
                       for s in range(G)]
                pos = lax.broadcasted_iota(jnp.int32, (nh, N), 1)
                scs = [jnp.where(pos < length(g * G + s), scs[s] * SCALE, -jnp.inf) for s in range(G)]
                ms = [jnp.max(sc, axis=-1, keepdims=True) for sc in scs]
                es = [jnp.exp(sc - m) for sc, m in zip(scs, ms)]
                ds = [jnp.sum(e, axis=-1, keepdims=True) for e in es]
                ps = [(e / d).astype(BF) for e, d in zip(es, ds)]
                outs = [lax.dot_general(ps[s], buf[slot, s, 0:LAT, 0:N], (((1,), (1,)), ((), ())),
                                        preferred_element_type=F32) for s in range(G)]
                for s in range(G):
                    row = lax.rem(bs[s], nb)
                    for i in range(LAT // 128):
                        o_s[pl.ds(row + i * nb, nh, stride=LAT // 128 * nb), :] = outs[s][:, i * 128:(i + 1) * 128]
        return carry

    lax.fori_loop(0, ng, body, 0)
    for h in range(nh):
        for i in range(LAT // 128):
            c = h * LAT + i * 128
            oflat[:, c:c + 128] = o_s[pl.ds((h * (LAT // 128) + i) * nb, nb), :].astype(BF)
    for g in range(ng if load else 0):
        wcopy(g).wait()
    nblk = 1024

    def mm(j, carry):
        cols = pl.ds(pl.multiple_of(j * nblk, nblk), nblk)
        out_ref[:, cols] = jnp.dot(oflat[...], wbuf[:, cols], preferred_element_type=F32)
        return carry
    lax.fori_loop(0, out_ref.shape[1] // nblk, mm, 0)


def _attention(layer, off, q, ct, order, wo, nh, G=8, NS=3):
    kv, s_len = ct.shape[2:]
    nb = order.shape[1] // 2
    hid, d = wo.shape[-2:]
    load = wo.ndim == 3
    part = jax.ShapeDtypeStruct((nb, d), F32)
    return pl.pallas_call(
        functools.partial(_attn_kernel, layer, off, load, nh, G, NS),
        out_shape=[part, jax.ShapeDtypeStruct((hid, d), BF)] if load else part,
        in_specs=[SMEM, VMEM, ANY, ANY if load else VMEM],
        out_specs=[VMEM, VMEM] if load else VMEM,
        scratch_shapes=[
            pltpu.VMEM((NS, G, kv, s_len), BF), pltpu.SemaphoreType.DMA((NS, G)),
            pltpu.VMEM((LAT // 128 * nb * nh, 128), F32), pltpu.VMEM((nb, hid), BF),
        ] + ([pltpu.SemaphoreType.DMA((nb // G,))] if load else []),
        compiler_params=pltpu.CompilerParams(vmem_limit_bytes=24 * 2 ** 20),
        cost_estimate=pl.CostEstimate(flops=20 * 10 ** 9, bytes_accessed=40 * 2 ** 20, transcendentals=0),
        name=f"attn{layer}",
    )(order, q, ct, wo)


XLOC = {1: (1, 0), 0: (2, 0)}
YLOC = {0: (1, 1), 1: (2, 1)}
W = 512
A = (0, 1)
B = (2, 3)
QORDER = (0, 2, 1, 3)
HALF = 64


def _ffn_kernel(layer, last, nh, xo_ref, pa_ref, pb_ref, fn_ref, an_ref, w1_ref, w3_ref, w2_ref, wq_ref, wo_ref, *rest):
    if last:
        out_ref, rest = rest[0], rest[1:]
    else:
        xn_ref, q_ref, won_ref, rest = rest[0], rest[1], rest[2], rest[3:]
    (w13, w2b, gbuf, ybuf, sbuf, abuf, xp, xall,
     r1x_own, r1x_y, r1y_own, r1y_x, r2x, r2y,
     wsem, w2sem, wqsem, wosem, ss, rs) = rest
    tp = lax.axis_index("tp")
    dp = lax.axis_index("dp")
    xi, ci = lax.div(dp, 2), lax.rem(dp, 2)
    SIB = (tp, xi * 2 + 1 - ci)
    X = (tp, (1 - xi) * 2 + ci)
    Y = (1 - tp, dp)

    bar = pltpu.get_barrier_semaphore()
    for peer in (SIB, X, Y):
        pl.semaphore_signal(bar, inc=1, device_id=peer, device_id_type=MESH)

    nblk = w1_ref.shape[2] // 128
    wcopies = []
    for j in range(nblk):
        for i, w in enumerate((w3_ref, w1_ref)):
            wcopies.append(pltpu.make_async_copy(
                w.at[layer, :, pl.ds(j * 128, 128)], w13.at[:, pl.ds(j * 256 + i * 128, 128)],
                wsem.at[j, i]))
    w2copy = pltpu.make_async_copy(w2_ref.at[layer], w2b.at[pl.ds(0, w2_ref.shape[1]), pl.ds(0, w2_ref.shape[2])], w2sem)
    for cp in wcopies:
        cp.start()
    w2copy.start()
    nj = nh // 2
    if not last:
        kv2 = wq_ref.shape[2] // nj
        dst = [(w13 if j < 2 else w2b).at[:, pl.ds(j % 2 * kv2, kv2)] for j in range(nj)]
        wqcopies = [pltpu.make_async_copy(wq_ref.at[layer + 1, :, pl.ds(j * kv2, kv2)], dst[j], wqsem.at[j])
                    for j in range(nj)]
        wocopy = pltpu.make_async_copy(wo_ref.at[layer + 1], won_ref, wosem)

    count = [16]

    def remote(src, dst, dev, i=None):
        if i is None:
            i = count[0]
            count[0] += 1
        return pltpu.make_async_remote_copy(src_ref=src, dst_ref=dst, send_sem=ss.at[i], recv_sem=rs.at[i],
                                            device_id=dev, device_id_type=MESH)

    def cols(q):
        return pl.ds(q * W, W)

    colA, colB = pl.ds(A[0] * W, len(A) * W), pl.ds(B[0] * W, len(B) * W)
    own_sib = remote(gbuf.at[0, 0], gbuf.at[0, 1], SIB)
    own_x = {p: remote(gbuf.at[0, 0, p], gbuf.at[XLOC[p][0], 0, XLOC[p][1]], X) for p in (1, 0)}
    own_y = {p: remote(gbuf.at[0, 0, p], gbuf.at[YLOC[p][0], 0, YLOC[p][1]], Y) for p in (0, 1)}
    relay_x = remote(gbuf.at[1, 0, 1], gbuf.at[3, 0, 0], X)
    relay_y = remote(gbuf.at[1, 0, 0], gbuf.at[3, 0, 1], Y)
    sib_g = {k: remote(gbuf.at[k, 0], gbuf.at[k, 1], SIB) for k in (1, 2, 3)}
    PS = (0, 1)
    st1_x = {p: remote(ybuf.at[XLOC[p][0], 0, XLOC[p][1], :, colA], r1x_own.at[p], X) for p in PS}
    st1_y = {p: remote(ybuf.at[YLOC[p][0], 0, YLOC[p][1], :, colB], r1y_own.at[p], Y) for p in PS}
    st1_dx = {(p, q): remote(ybuf.at[3, 0, p, :, cols(q)], r1x_y.at[p, i], X) for p in PS for i, q in enumerate(A)}
    st1_dy = {(p, q): remote(ybuf.at[3, 0, p, :, cols(q)], r1y_x.at[p, i], Y) for p in PS for i, q in enumerate(B)}
    st2_y = {(p, q): remote(r1x_y.at[p, i], r2y.at[p, i], Y) for p in PS for i, q in enumerate(A)}
    st2_x = {(p, q): remote(r1y_x.at[p, i], r2x.at[p, i], X) for p in PS for i, q in enumerate(B)}
    mine = [pl.ds(pl.multiple_of(tp * HALF + p * 32, 32), 32) for p in PS]
    xg = {(p, q): remote(xall.at[mine[p], cols(q)], xall.at[mine[p], cols(q)], Y) for p in PS for q in A + B}

    def sib_y(k, q):
        return remote(ybuf.at[k, 1, :, :, cols(q)], sbuf.at[k, :, :, cols(q)], SIB, k * 4 + q)

    if xo_ref.shape[0] == HALF:
        xo = xo_ref[...]
    else:
        xo = xo_ref[pl.ds(pl.multiple_of(tp * HALF, HALF), HALF), :]
    x1 = (xo.astype(F32) + (pa_ref[...] + pb_ref[...]).astype(BF).astype(F32)).astype(BF)
    xp[...] = x1
    gbuf[0, 0] = _rmsnorm(x1, fn_ref[layer:layer + 1, :]).reshape(2, 32, -1)

    pl.semaphore_wait(bar, 3)
    own_sib.start()
    own_x[1].start()
    own_y[0].start()
    own_x[0].start()
    own_y[1].start()

    def combine(k, q):
        sib_y(k, q).wait_recv()
        ybuf[k, 0, :, :, cols(q)] = ybuf[k, 0, :, :, cols(q)] + sbuf[k, :, :, cols(q)]

    def chunk(k, carry):
        @pl.when(k == 0)
        def _():
            own_sib.wait_recv()
            for cp in wcopies:
                cp.wait()
        for kk in (1, 2, 3):
            @pl.when(k == kk)
            def _():
                sib_g[kk].wait_recv()
        g = gbuf[k].reshape(2 * HALF, -1)
        for j in range(nblk):
            uv = jnp.dot(g, w13[:, j * 256:(j + 1) * 256], preferred_element_type=F32)
            u, v = uv[:, :128], uv[:, 128:]
            abuf[:, j * 128:(j + 1) * 128] = (jax.nn.silu(u) * v).astype(BF)

        @pl.when(k == 0)
        def _():
            own_x[1].wait_recv()
            own_y[0].wait_recv()
            relay_x.start()
            relay_y.start()
            sib_g[1].start()
            w2copy.wait()

        @pl.when(k == 1)
        def _():
            own_x[0].wait_recv()
            own_y[1].wait_recv()
            sib_g[2].start()
            for q in QORDER:
                combine(0, q)

        @pl.when(k == 2)
        def _():
            relay_x.wait_recv()
            relay_y.wait_recv()
            sib_g[3].start()
            for q in QORDER:
                combine(1, q)
            st1_x[1].start()
            st1_y[0].start()

        @pl.when(k == 3)
        def _():
            if not last:
                for cp in wqcopies[:2]:
                    cp.start()
            for q in QORDER:
                combine(2, q)
            st1_x[0].start()
            st1_y[1].start()

        a = abuf[...]
        for q in QORDER:
            y = jnp.dot(a, w2b[0:w2_ref.shape[1], q * W:(q + 1) * W], preferred_element_type=F32)
            ybuf[k, :, :, :, q * W:(q + 1) * W] = y.reshape(2, 2, 32, W)
            sib_y(k, q).start()
        return carry

    lax.fori_loop(0, 4, chunk, 0)
    if not last:
        for cp in wqcopies[2:]:
            cp.start()
        wocopy.start()
    for q in QORDER:
        combine(3, q)
        for p in PS:
            (st1_dx if q in A else st1_dy)[p, q].start()
    for q in QORDER:
        for p in PS:
            if q in A:
                st1_dx[p, q].wait_recv()
                (k, j), i = YLOC[p], A.index(q)
                r1x_y[p, i] = r1x_y[p, i] + ybuf[k, 0, j, :, q * W:(q + 1) * W]
                st2_y[p, q].start()
            else:
                st1_dy[p, q].wait_recv()
                (k, j), i = XLOC[p], B.index(q)
                r1y_x[p, i] = r1y_x[p, i] + ybuf[k, 0, j, :, q * W:(q + 1) * W]
                st2_x[p, q].start()
    for p in PS:
        st1_x[p].wait_recv()
        st1_y[p].wait_recv()
    for q in QORDER:
        for p in PS:
            c = slice(q * W, (q + 1) * W)
            y = ybuf[0, 0, p, :, c]
            if q in A:
                st2_y[p, q].wait_recv()
                i = A.index(q)
                y = y + r1x_own[p, :, i * W:(i + 1) * W] + r2y[p, i]
            else:
                st2_x[p, q].wait_recv()
                i = B.index(q)
                y = y + r1y_own[p, :, i * W:(i + 1) * W] + r2x[p, i]
            xn = (xp[p * 32:(p + 1) * 32, c].astype(F32) + y.astype(BF).astype(F32)).astype(BF)
            xall[mine[p], c] = xn
            if not last:
                xn_ref[p * 32:(p + 1) * 32, c] = xn
            xg[p, q].start()
    for cp in xg.values():
        cp.wait_recv()
    if last:
        out_ref[...] = xall[...]
    else:
        h = _rmsnorm(xall[...], an_ref[layer + 1:layer + 2, :])
        for j, cp in enumerate(wqcopies):
            cp.wait()
            _project(h, dst[j][...], j, q_ref, 2 * HALF, kv2 // 2)
    if not last:
        wocopy.wait()
    for cp in [own_sib, relay_x, relay_y, *own_x.values(), *own_y.values(), *sib_g.values(),
               *st1_x.values(), *st1_y.values(), *st1_dx.values(), *st1_dy.values(),
               *st2_x.values(), *st2_y.values(), *xg.values()]:
        cp.wait_send()
    for k in range(4):
        for q in QORDER:
            sib_y(k, q).wait_send()


NCOPY = 16 + 10 + 4 + 8 + 8 + 8


def _ffn(layer, last, nh, xo, pa, pb, fn, an, w1, w3, w2, wq, wo):
    rows, d = pa.shape
    f = w1.shape[2]
    kv = wq.shape[2] // nh
    if last:
        out_shape = [jax.ShapeDtypeStruct((2 * rows, d), BF)]
    else:
        out_shape = [jax.ShapeDtypeStruct((rows, d), BF),
                     jax.ShapeDtypeStruct((-(-kv // 128) * 2 * rows * nh, 128), F32),
                     jax.ShapeDtypeStruct(wo.shape[1:], BF)]
    NA, NB = len(A), len(B)
    scratch = [
        pltpu.VMEM((d, 2 * f), BF), pltpu.VMEM((f, d) if last else (d, 4 * kv), BF),
        pltpu.VMEM((4, 2, 2, 32, d), BF), pltpu.VMEM((4, 2, 2, 32, d), F32), pltpu.VMEM((4, 2, 32, d), F32),
        pltpu.VMEM((128, f), BF), pltpu.VMEM((rows, d), BF), pltpu.VMEM((2 * rows, d), BF),
        pltpu.VMEM((2, 32, NA * W), F32), pltpu.VMEM((2, NA, 32, W), F32),
        pltpu.VMEM((2, 32, NB * W), F32), pltpu.VMEM((2, NB, 32, W), F32),
        pltpu.VMEM((2, NB, 32, W), F32), pltpu.VMEM((2, NA, 32, W), F32),
        pltpu.SemaphoreType.DMA((f // 128, 2)), pltpu.SemaphoreType.DMA, pltpu.SemaphoreType.DMA((nh // 2,)),
        pltpu.SemaphoreType.DMA, pltpu.SemaphoreType.DMA((NCOPY,)), pltpu.SemaphoreType.DMA((NCOPY,)),
    ]
    return pl.pallas_call(
        functools.partial(_ffn_kernel, layer, last, nh),
        out_shape=out_shape,
        in_specs=[VMEM, VMEM, VMEM, VMEM, VMEM, ANY, ANY, ANY, ANY, ANY],
        out_specs=[VMEM] * len(out_shape),
        scratch_shapes=scratch,
        compiler_params=pltpu.CompilerParams(collective_id=layer, has_side_effects=True,
                                             vmem_limit_bytes=65 * 2 ** 19),
        name=f"ffn{layer}",
    )(xo, pa, pb, fn, an, w1, w3, w2, wq, wo)


def solution(mesh):
    def body(x, lengths, cache, attn_norm, ffn_norm, wq, wo, w1, w3, w2):
        nb = x.shape[0]
        n_layers, _, s_len, kv = cache.shape
        nh = wq.shape[2] // kv
        ct = jnp.swapaxes(cache, 2, 3)
        ct, wq, wo, w1, w3, w2 = [pltpu.with_memory_space_constraint(t, pltpu.HBM) for t in (ct, wq, wo, w1, w3, w2)]
        order, q = _first(lengths, x, attn_norm, wq, nh)
        for l in range(n_layers):
            last = l == n_layers - 1
            if l == 0:
                pa, wo_l = _attention(l, 0, q, ct, order, wo, nh)
            else:
                pa = _attention(l, 0, q, ct, order, wo_l, nh)
            pa = lax.ppermute(pa, 'tp', [(0, 1), (1, 0)])
            pb = _attention(l, nb // 2, q, ct, order, wo_l, nh)
            res = _ffn(l, last, nh, x, pb, pa, ffn_norm, attn_norm, w1, w3, w2, wq, wo)
            if last:
                return res[0]
            x, q, wo_l = res

    in_specs = (
        P('dp', None),
        P('dp'),
        P(None, 'dp', None, None),
        P(None, None),
        P(None, None),
        P(None, None, 'tp'),
        P(None, 'tp', None),
        P(None, None, ('dp', 'tp')),
        P(None, None, ('dp', 'tp')),
        P(None, ('dp', 'tp'), None),
    )
    return jax.shard_map(body, mesh=mesh, in_specs=in_specs, out_specs=P('dp', None), check_vma=False)
```
